128 devices in a mesh: cand: 8 (over z, y_hi), ground: 16 (over x, y_lo, core).
Axes of the slice: x: 4, y: 4 (y_hi: 2, y_lo: 2; y = y_hi * 2 + y_lo), z: 4, core: 2. Of those that a mesh axis runs over, the one named last changes fastest.
Arguments:
- ground_rows: bfloat16 [131072, 1024], P('ground'), may hold values from -6 to 6
- best: float32 [131072], P('ground'), may hold values from -1.9 to 1.4
- cand_index: int32 [8192], P('cand'), may hold values from 0 to 131071
- chosen_index: int32 [64], replicated, may hold values from 0 to 131071
Outputs:
- gains: float32 [8192], P(('cand', 'ground'))
- new_best: float32 [131072], P('ground')
The draws below stay inside these ranges and needn't reach their ends.
All inputs are finite; a program needn't handle non-finite values.
Results may differ from the reference program's by a relative error of at most 0.0003.
Values may be sent and summed in bfloat16 or wider, within the bound.
No kernel may reach another device: no remote copies, remote signals or barrier semaphores. Data moves between devices by JAX's collectives and lax.ppermute only.
A program may use at most 64 MiB of HBM per device.

```python
import jax
import jax.numpy as jnp
from jax import lax

D = 1024
CHOSEN = 64
C = 8192
G = 131072


def draw_ground_rows(key, part):
    groups = max(G // 1024, 8)
    base = jax.random.fold_in(key, 17)
    key_centre, key_weight, key_label, key_noise = jax.random.split(base, 4)
    centres = jax.random.normal(key_centre, (groups, D), jnp.float32)
    label = jax.random.randint(key_label, (G,), 0, groups)
    weight = jax.random.uniform(key_weight, (groups,), jnp.float32, 0.05, 0.4)
    noise = jax.random.normal(key_noise, (G, D), jnp.float32)
    share = jnp.take(weight, label, axis=0)[:, None]
    rows = jnp.sqrt(share) * jnp.take(centres, label, axis=0) + jnp.sqrt(1.0 - share) * noise
    return jnp.clip(rows, -6.0, 6.0).astype(jnp.bfloat16)


def draw_best(key, part):
    place = jnp.arange(G).astype(jnp.float32) / G
    noise = jax.random.uniform(key, (G,), jnp.float32, -0.5, 0.5)
    return 1.5 * place - 1.0 + noise


def touch_ends(values, key, low, largest):
    index_at = [jax.random.randint(jax.random.fold_in(key, axis), (), 0, length) for axis, length in enumerate(values.shape)]
    main_axis = values.shape.index(max(values.shape))
    next_to = index_at[:main_axis] + [(index_at[main_axis] + 1) % values.shape[main_axis]] + index_at[main_axis + 1:]
    return values.at[tuple(index_at)].set(low).at[tuple(next_to)].set(largest)


def setup_inputs(seed: int = 0) -> dict:
    key_list = jax.random.split(jax.random.key(seed), 5)
    return {
        "ground_rows": draw_ground_rows(jax.random.fold_in(key_list[4], 71), 0),
        "best": draw_best(jax.random.fold_in(key_list[4], 71), 0),
        "cand_index": touch_ends(jax.random.randint(key_list[2], (C,), 0, G), jax.random.fold_in(key_list[2], 1), 0, G - 1).astype(jnp.int32),
        "chosen_index": touch_ends(jax.random.randint(key_list[3], (CHOSEN,), 0, G), jax.random.fold_in(key_list[3], 1), 0, G - 1).astype(jnp.int32),
    }


def reference(ground_rows, best, cand_index, chosen_index):
    scale = D ** -0.5
    cand_rows = jnp.take(ground_rows, cand_index, axis=0)
    chosen_rows = jnp.take(ground_rows, chosen_index, axis=0)
    block = min(1024, G)
    slabs = ground_rows.reshape(G // block, block, D)
    bests = best.reshape(G // block, block)

    def step(total, pair):
        slab, level = pair
        sims = jnp.dot(cand_rows, slab.T, preferred_element_type=jnp.float32) * scale
        total = total + jnp.sum(jnp.maximum(sims - level[None, :], 0.0), axis=1)
        near = jnp.dot(chosen_rows, slab.T, preferred_element_type=jnp.float32) * scale
        return total, jnp.maximum(level, jnp.max(near, axis=0))

    total, updated = lax.scan(step, jnp.zeros((C,), jnp.float32), (slabs, bests))
    return total / G, updated.reshape(G)
```

```python
import jax
import jax.numpy as jnp
from jax import lax
from jax.experimental import pallas as pl
from jax.experimental.pallas import tpu as pltpu
from jax.sharding import PartitionSpec as P

CAP = 96
CAP_CHOSEN = 16
SLOTS = CAP + CAP_CHOSEN
LANES = 128
TILE = 8

F32 = jnp.float32
BF16 = jnp.bfloat16
I32 = jnp.int32


def iota(shape, dim):
    return lax.broadcasted_iota(I32, shape, dim)


def pick_kernel(turn_ref, cand_ref, chosen_ref, slab_ref, block_ref, rank_ref, crank_ref, counts_ref,
                pad_ref, list_ref, slots_ref, stage_ref, sem, list_sem):
    count = slab_ref.shape[0]
    shift = count.bit_length() - 1
    me = lax.axis_index("ground")
    turn = turn_ref[0]
    lane = iota((LANES, LANES), 1)
    lower = jnp.where(iota((LANES, LANES), 0) >= lane, 1.0, 0.0).astype(BF16)

    def ranked(col, carry):
        slab = lax.shift_right_arithmetic(col, shift)
        hot = slab == lane
        upto = jnp.dot(lower, jnp.where(hot, 1.0, 0.0).astype(BF16), preferred_element_type=F32)
        rank = jnp.sum(jnp.where(hot, upto - 1.0 + carry, 0.0), axis=1, keepdims=True)
        return slab, rank, carry + upto[LANES - 1 : LANES, :]

    rows = cand_ref.shape[0]
    cand = cand_ref[...].T
    carry = jnp.zeros((1, LANES), F32)
    found = jnp.zeros((LANES, LANES), F32)
    ranks = []
    for j in range(rows):
        col = cand[:, j : j + 1]
        slab, rank, carry = ranked(col, carry)
        ranks.append(rank)
        slot = jnp.where(slab == me, rank.astype(I32) - turn * CAP, -1)
        hit = (slot == lane) & (lane < CAP)
        found += jnp.where(hit, (col - me * count).astype(F32), 0.0)
    counts = carry
    slots = jnp.concatenate(ranks, axis=1)
    rank_ref[...] = slots.T.astype(I32)

    pad_ref[...] = jnp.full(pad_ref.shape, -1, I32)
    pad_ref[0:1, 0 : chosen_ref.shape[1]] = chosen_ref[...]
    col = pad_ref[...].T[:, 0:1]
    slab, rank, ccounts = ranked(col, jnp.zeros((1, LANES), F32))
    slot = jnp.where(slab == me, rank.astype(I32) - turn * CAP_CHOSEN, -1)
    hit = (slot + CAP == lane) & (slot >= 0) & (lane < SLOTS)
    found += jnp.where(hit, (col - me * count).astype(F32), 0.0)
    crank_ref[...] = jnp.broadcast_to(rank, (LANES, 8)).T.astype(I32)
    counts_ref[...] = jnp.concatenate(
        [counts, ccounts, jnp.zeros((6, LANES), F32)], axis=0
    ).astype(I32)

    row = jnp.broadcast_to(jnp.sum(found, axis=0, keepdims=True), (8, LANES))
    list_ref[...] = row.astype(I32)
    copy = pltpu.make_async_copy(list_ref, slots_ref, list_sem)
    copy.start()
    copy.wait()
    for p in range(SLOTS):
        tile = lax.shift_right_logical(slots_ref[0, p], 3)
        pltpu.make_async_copy(slab_ref.at[pl.ds(pl.multiple_of(tile * TILE, TILE), TILE), :],
                              stage_ref.at[pl.ds(p * TILE, TILE), :], sem).start()
    inner = row.T[:, 0:1].astype(I32) & (TILE - 1)
    want = inner[:SLOTS] + TILE * iota((SLOTS, 1), 0)
    one = jnp.where(iota((SLOTS, SLOTS * TILE), 1) == want, 1.0, 0.0).astype(BF16)
    pltpu.make_async_copy(slab_ref.at[pl.ds(0, SLOTS * TILE), :], stage_ref, sem).wait()
    block_ref[...] = jnp.dot(one, stage_ref[...], preferred_element_type=F32).astype(BF16)


def pick(turn, cand, chosen, slab):
    width = slab.shape[1]
    return pl.pallas_call(
        pick_kernel,
        in_specs=[pl.BlockSpec(memory_space=pltpu.SMEM), pl.BlockSpec(memory_space=pltpu.VMEM),
                  pl.BlockSpec(memory_space=pltpu.VMEM), pl.BlockSpec(memory_space=pl.ANY)],
        out_specs=[pl.BlockSpec(memory_space=pltpu.VMEM)] * 4,
        out_shape=[jax.ShapeDtypeStruct((SLOTS, width), BF16),
                   jax.ShapeDtypeStruct(cand.shape, I32),
                   jax.ShapeDtypeStruct((8, LANES), I32),
                   jax.ShapeDtypeStruct((8, LANES), I32)],
        scratch_shapes=[pltpu.VMEM((8, LANES), I32), pltpu.VMEM((8, LANES), I32),
                        pltpu.SMEM((8, LANES), I32), pltpu.VMEM((SLOTS * TILE, width), BF16),
                        pltpu.SemaphoreType.DMA, pltpu.SemaphoreType.DMA],
        name="pick",
    )(turn, cand, chosen, slab)


def gain_kernel(order_ref, turn_ref, counts_ref, cand_ref, rank_ref, before_ref, best_ref, slab_ref, *rest,
                steps, peers, shift, scale):
    blocks = rest[:peers]
    out_ref, recv_ref, dense_ref, acc_ref, starts_ref, sem = rest[peers:]
    step = pl.program_id(0)
    total = dense_ref.shape[0] - 2 * SLOTS
    turn = turn_ref[0]

    @pl.when(step == 0)
    def _():
        for a in range(peers):
            pltpu.make_async_copy(blocks[a], recv_ref.at[pl.ds(a * SLOTS, SLOTS), :], sem).start()
        start = jnp.int32(0)
        for a in range(peers):
            starts_ref[a] = start
            here = counts_ref[0, order_ref[a]] - turn * CAP
            starts_ref[peers + a] = jnp.clip(here, 0, CAP)
            start = start + jnp.clip(here, 0, CAP)
        dense_ref[...] = jnp.zeros_like(dense_ref)
        acc_ref[...] = jnp.zeros_like(acc_ref)
        pltpu.make_async_copy(recv_ref, recv_ref, sem).wait()
        q = iota((1, 2 * SLOTS), 1)
        for a in range(0, peers, 2):
            base = pl.multiple_of(starts_ref[a] // 16 * 16, 16)
            first = jnp.where(q < starts_ref[peers + a], q + starts_ref[a], -1)
            late = q - SLOTS
            second = jnp.where(late < starts_ref[peers + a + 1], late + starts_ref[a + 1], -1)
            target = jnp.where(q < SLOTS, first, second)
            at = iota((2 * SLOTS, 1), 0) + base
            one = jnp.where(at == target, 1.0, 0.0).astype(BF16)
            rows = jnp.dot(one, recv_ref[pl.ds(a * SLOTS, 2 * SLOTS), :], preferred_element_type=F32)
            window = pl.ds(base, 2 * SLOTS)
            dense_ref[window, :] = (dense_ref[window, :].astype(F32) + rows).astype(BF16)

    level = best_ref[...] * (1.0 / scale)
    sub = 256
    for u in range(slab_ref.shape[0] // sub):
        sims = lax.dot_general(dense_ref[pl.ds(0, total), :], slab_ref[pl.ds(u * sub, sub), :],
                               (((1,), (1,)), ((), ())), preferred_element_type=F32)
        part = acc_ref[...]
        for j in range(sub // LANES):
            edge = level[u * (sub // LANES) + j : u * (sub // LANES) + j + 1, :]
            part += jnp.maximum(sims[:, j * LANES : (j + 1) * LANES] - edge, 0.0)
        acc_ref[...] = part

    @pl.when(step == steps - 1)
    def _():
        sums = jnp.sum(acc_ref[...], axis=1, keepdims=True) * scale
        slab = lax.shift_right_arithmetic(cand_ref[...], shift)
        slot = rank_ref[...] - turn * CAP
        place = jnp.full(slot.shape, -1, I32)
        for a in range(peers):
            place = jnp.where(slab == order_ref[a], slot + starts_ref[a], place)
        place = jnp.where((slot >= 0) & (slot < CAP), place, -1)
        at = iota((total, LANES), 0)
        for j in range(slot.shape[0]):
            mine = jnp.where(at == place[j : j + 1, :], sums, 0.0)
            out_ref[j : j + 1, :] = before_ref[j : j + 1, :] + jnp.sum(mine, axis=0, keepdims=True)


def gain(order, turn, counts, cand, rank, before, best, slab, blocks, scale):
    count, width = slab.shape
    total = cand.shape[0] * cand.shape[1]
    peers = len(blocks)
    tall = min(1024, count)
    steps = count // tall
    whole = lambda i: (0, 0)
    body = lambda *refs: gain_kernel(*refs, steps=steps, peers=peers, shift=count.bit_length() - 1, scale=scale)
    return pl.pallas_call(
        body,
        grid=(steps,),
        in_specs=[pl.BlockSpec(memory_space=pltpu.SMEM)] * 3
        + [pl.BlockSpec(cand.shape, whole)] * 3
        + [pl.BlockSpec((tall // LANES, LANES), lambda i: (i, 0)), pl.BlockSpec((tall, width), lambda i: (i, 0))]
        + [pl.BlockSpec(memory_space=pl.ANY)] * peers,
        out_specs=pl.BlockSpec(cand.shape, whole),
        out_shape=jax.ShapeDtypeStruct(cand.shape, F32),
        scratch_shapes=[pltpu.VMEM((peers * SLOTS, width), BF16),
                        pltpu.VMEM((total + 2 * SLOTS, width), BF16),
                        pltpu.VMEM((total, LANES), F32),
                        pltpu.SMEM((2 * peers,), I32),
                        pltpu.SemaphoreType.DMA],
        compiler_params=pltpu.CompilerParams(vmem_limit_bytes=48 * 2**20, dimension_semantics=("arbitrary",)),
        name="gain",
    )(order, turn, counts, cand, rank, before, best, slab, *blocks)


def near_kernel(order_ref, turn_ref, counts_ref, best_ref, slab_ref, *rest, peers, scale):
    blocks = rest[:peers]
    out_ref, recv_ref, dense_ref, sem = rest[peers:]
    width = slab_ref.shape[1]
    turn = turn_ref[0]
    chosen = dense_ref.shape[0]

    @pl.when(pl.program_id(0) == 0)
    def _():
        for a in range(peers):
            pltpu.make_async_copy(blocks[a].at[pl.ds(CAP, CAP_CHOSEN), :],
                                  recv_ref.at[pl.ds(a * CAP_CHOSEN, CAP_CHOSEN), :], sem).start()
        q = iota((1, peers * CAP_CHOSEN), 1)
        target = jnp.full((1, peers * CAP_CHOSEN), -1, I32)
        start = jnp.int32(0)
        for a in range(peers):
            here = jnp.clip(counts_ref[1, order_ref[a]] - turn * CAP_CHOSEN, 0, CAP_CHOSEN)
            slot = q - a * CAP_CHOSEN
            target = jnp.where((slot >= 0) & (slot < here), slot + start, target)
            start = start + here
        one = jnp.where(iota((chosen, 1), 0) == target, 1.0, 0.0).astype(BF16)
        pltpu.make_async_copy(recv_ref, recv_ref, sem).wait()
        dense_ref[...] = jnp.dot(one, recv_ref[...], preferred_element_type=F32).astype(BF16)

    there = jnp.int32(0)
    for a in range(peers):
        there = there + jnp.clip(counts_ref[1, order_ref[a]] - turn * CAP_CHOSEN, 0, CAP_CHOSEN)
    sims = lax.dot_general(dense_ref[...], slab_ref[...], (((1,), (1,)), ((), ())),
                           preferred_element_type=F32) * scale
    low = jnp.where(iota((chosen, 1), 0) < there, 0.0, -jnp.inf)
    top = jnp.max(sims + low, axis=0, keepdims=True)
    for j in range(out_ref.shape[0]):
        out_ref[j : j + 1, :] = jnp.maximum(best_ref[j : j + 1, :], top[:, j * LANES : (j + 1) * LANES])


def near(order, turn, counts, best, slab, blocks, chosen, scale):
    count, width = slab.shape
    peers = len(blocks)
    tall = min(1024, count)
    body = lambda *refs: near_kernel(*refs, peers=peers, scale=scale)
    level = pl.BlockSpec((tall // LANES, LANES), lambda i: (i, 0))
    return pl.pallas_call(
        body,
        grid=(count // tall,),
        in_specs=[pl.BlockSpec(memory_space=pltpu.SMEM)] * 3
        + [level, pl.BlockSpec((tall, width), lambda i: (i, 0))]
        + [pl.BlockSpec(memory_space=pl.ANY)] * peers,
        out_specs=level,
        out_shape=jax.ShapeDtypeStruct(best.shape, F32),
        scratch_shapes=[pltpu.VMEM((peers * CAP_CHOSEN, width), BF16),
                        pltpu.VMEM((chosen, width), BF16), pltpu.SemaphoreType.DMA],
        compiler_params=pltpu.CompilerParams(vmem_limit_bytes=32 * 2**20, dimension_semantics=("arbitrary",)),
        name="near",
    )(order, turn, counts, best, slab, *blocks)


def device(x, y, c):
    return (x % 4) * 4 + y * 2 + c


def moved(array, dx, dy, dc):
    pairs = [(device(x, y, c), device(x + (dx if c == 0 else -dx), y ^ dy, c ^ dc))
             for x in range(4) for y in range(2) for c in range(2)]
    return lax.ppermute(array, "ground", pairs)


def spread(own):
    me = lax.axis_index("ground")
    x, y, c = me // 4, me // 2 % 2, me % 2
    flip = moved(own, 0, 1, 0)
    ahead = moved(own, 1, 0, 0)
    behind = moved(own, -1, 0, 0)
    across = moved(ahead, 1, 0, 0)
    flip_ahead = moved(flip, 1, 0, 0)
    flip_behind = moved(flip, -1, 0, 0)
    flip_across = moved(across, 0, 1, 0)
    mine = [own, flip, ahead, behind, across, flip_ahead, flip_behind, flip_across]
    sign = 1 - 2 * c
    where = [(0, y), (0, 1 - y), (-sign, y), (sign, y), (2, y), (-sign, 1 - y), (sign, 1 - y), (2, 1 - y)]
    here = [(x + dx) % 4 * 4 + yy * 2 + c for dx, yy in where]
    there = [(x - dx) % 4 * 4 + yy * 2 + 1 - c for dx, yy in where]
    theirs = [moved(block, 0, 0, 1) for block in mine]
    return mine + theirs, jnp.stack(here + there).astype(I32)


def body(ground_rows, best, cand_index, chosen_index):
    count, width = ground_rows.shape
    scale = width ** (-0.5)
    peers = lax.axis_size("ground")
    whole = count * peers
    cand = cand_index.reshape(-1, LANES)
    chosen = chosen_index.reshape(1, -1)
    level = best.reshape(-1, LANES)

    def exchange(turn, gains, level):
        turn = turn.reshape(1)
        block, rank, crank, counts = pick(turn, cand, chosen, ground_rows)
        blocks, order = spread(block)
        counts_row = counts
        gains = gain(order, turn, counts_row, cand, rank, gains, best.reshape(-1, LANES), ground_rows, blocks, scale)
        level = near(order, turn, counts_row, level, ground_rows, blocks, chosen.shape[1], scale)
        return gains, level, counts

    gains, level, counts = exchange(jnp.int32(0), jnp.zeros(cand.shape, F32), level)
    turns = jnp.maximum(
        (jnp.max(counts[0]) + CAP - 1) // CAP, (jnp.max(counts[1]) + CAP_CHOSEN - 1) // CAP_CHOSEN
    )

    def more(state):
        return state[0] < turns

    def again(state):
        gains, level, unused = exchange(state[0], state[1], state[2])
        return state[0] + 1, gains, level

    unused, gains, level = lax.while_loop(more, again, (jnp.int32(1), gains, level))
    blocks = gains.reshape(peers, -1) / whole
    arrived = lax.all_to_all(blocks, "ground", 0, 0, tiled=True)
    return arrived.sum(axis=0), level.reshape(-1)


def solution(mesh):
    in_specs = (P("ground", None), P("ground"), P("cand"), P())
    out_specs = (P(("cand", "ground")), P("ground"))
    return jax.shard_map(body, mesh=mesh, in_specs=in_specs, out_specs=out_specs, check_vma=False)
```

```python
import jax
import jax.numpy as jnp
from jax import lax
from jax.experimental import pallas as pl
from jax.experimental.pallas import tpu as pltpu
from jax.sharding import PartitionSpec as P

CAP = 96
CAP_CHOSEN = 16
SLOTS = CAP + CAP_CHOSEN
LANES = 128
TILE = 8

F32 = jnp.float32
BF16 = jnp.bfloat16
I32 = jnp.int32


def iota(shape, dim):
    return lax.broadcasted_iota(I32, shape, dim)


def pick_kernel(turn_ref, cand_ref, chosen_ref, slab_ref, block_ref, rank_ref, counts_ref,
                pad_ref, list_ref, slots_ref, stage_ref, sem, list_sem):
    count = slab_ref.shape[0]
    shift = count.bit_length() - 1
    me = lax.axis_index("ground")
    turn = turn_ref[0]
    lane = iota((LANES, LANES), 1)
    lower = jnp.where(iota((LANES, LANES), 0) >= lane, 1.0, 0.0).astype(BF16)

    def ranked(col, carry):
        slab = lax.shift_right_arithmetic(col, shift)
        hot = slab == lane
        upto = jnp.dot(lower, jnp.where(hot, 1.0, 0.0).astype(BF16), preferred_element_type=F32)
        rank = jnp.sum(jnp.where(hot, upto - 1.0 + carry, 0.0), axis=1, keepdims=True)
        return slab, rank, carry + upto[LANES - 1 : LANES, :]

    rows = cand_ref.shape[0]
    cand = cand_ref[...].T
    carry = jnp.zeros((1, LANES), F32)
    found = jnp.zeros((LANES, LANES), F32)
    ranks = []
    for j in range(rows):
        col = cand[:, j : j + 1]
        slab, rank, carry = ranked(col, carry)
        ranks.append(rank)
        slot = jnp.where(slab == me, rank.astype(I32) - turn * CAP, -1)
        hit = (slot == lane) & (lane < CAP)
        found += jnp.where(hit, (col - me * count).astype(F32), 0.0)
    counts = carry
    slots = jnp.concatenate(ranks, axis=1)
    rank_ref[...] = slots.T.astype(I32)

    pad_ref[...] = jnp.full(pad_ref.shape, -1, I32)
    pad_ref[0:1, 0 : chosen_ref.shape[1]] = chosen_ref[...]
    col = pad_ref[...].T[:, 0:1]
    slab, rank, ccounts = ranked(col, jnp.zeros((1, LANES), F32))
    slot = jnp.where(slab == me, rank.astype(I32) - turn * CAP_CHOSEN, -1)
    hit = (slot + CAP == lane) & (slot >= 0) & (lane < SLOTS)
    found += jnp.where(hit, (col - me * count).astype(F32), 0.0)
    turns = jnp.maximum(
        (jnp.max(counts, axis=1, keepdims=True).astype(I32) + CAP - 1) // CAP,
        (jnp.max(ccounts, axis=1, keepdims=True).astype(I32) + CAP_CHOSEN - 1) // CAP_CHOSEN,
    )
    counts_ref[0:1, :] = counts.astype(I32)
    counts_ref[1:2, :] = ccounts.astype(I32)
    counts_ref[2:3, :] = jnp.broadcast_to(turns, (1, LANES))

    row = jnp.broadcast_to(jnp.sum(found, axis=0, keepdims=True), (8, LANES))
    list_ref[...] = row.astype(I32)
    copy = pltpu.make_async_copy(list_ref, slots_ref, list_sem)
    copy.start()
    copy.wait()
    for p in range(SLOTS):
        tile = lax.shift_right_logical(slots_ref[0, p], 3)
        pltpu.make_async_copy(slab_ref.at[pl.ds(pl.multiple_of(tile * TILE, TILE), TILE), :],
                              stage_ref.at[pl.ds(p * TILE, TILE), :], sem).start()
    inner = row.T[:, 0:1].astype(I32) & (TILE - 1)
    want = inner[:SLOTS] + TILE * iota((SLOTS, 1), 0)
    one = jnp.where(iota((SLOTS, SLOTS * TILE), 1) == want, 1.0, 0.0).astype(BF16)
    pltpu.make_async_copy(slab_ref.at[pl.ds(0, SLOTS * TILE), :], stage_ref, sem).wait()
    block_ref[...] = jnp.dot(one, stage_ref[...], preferred_element_type=F32).astype(BF16)


def pick(turn, cand, chosen, slab):
    width = slab.shape[1]
    return pl.pallas_call(
        pick_kernel,
        in_specs=[pl.BlockSpec(memory_space=pltpu.SMEM), pl.BlockSpec(memory_space=pltpu.VMEM),
                  pl.BlockSpec(memory_space=pltpu.VMEM), pl.BlockSpec(memory_space=pl.ANY)],
        out_specs=[pl.BlockSpec(memory_space=pltpu.VMEM)] * 3,
        out_shape=[jax.ShapeDtypeStruct((SLOTS, width), BF16),
                   jax.ShapeDtypeStruct(cand.shape, I32),
                   jax.ShapeDtypeStruct((8, LANES), I32)],
        scratch_shapes=[pltpu.VMEM((8, LANES), I32), pltpu.VMEM((8, LANES), I32),
                        pltpu.SMEM((8, LANES), I32), pltpu.VMEM((SLOTS * TILE, width), BF16),
                        pltpu.SemaphoreType.DMA, pltpu.SemaphoreType.DMA],
        name="pick",
    )(turn, cand, chosen, slab)


def gain_kernel(turn_ref, counts_ref, cand_ref, rank_ref, before_ref, best_ref, slab_ref, *rest,
                peers, earlier, main, last, scale):
    blocks = rest[:peers]
    if last:
        out_ref, level_ref, dense_ref, acc_ref, at_ref, tall_ref, sems = rest[peers:]
    else:
        out_ref, dense_ref, acc_ref, at_ref, tall_ref, sems = rest[peers:]
        level_ref = None
    chunks, chunk, width = tall_ref.shape
    count = slab_ref.shape[0]
    shift = count.bit_length() - 1
    total = cand_ref.shape[0] * cand_ref.shape[1]
    head = dense_ref.shape[0] - 2 * SLOTS - (total if last else main)
    turn = turn_ref[0]
    for i in range(chunks):
        pltpu.make_async_copy(slab_ref.at[pl.ds(i * chunk, chunk), :], tall_ref.at[i], sems.at[i]).start()

    sources = arrivals()[:peers]
    start = jnp.int32(0)
    done = jnp.int32(0)
    starts, heres = [], []
    for a in range(peers):
        if a == earlier:
            done = jnp.minimum(start, turn_ref[1])
        here = jnp.clip(counts_ref[0, sources[a]] - turn * CAP, 0, CAP)
        starts.append(start)
        heres.append(here)
        start = start + here
    stop = start if last else jnp.minimum(start, main)

    dense_ref[...] = jnp.zeros_like(dense_ref)
    acc_ref[...] = jnp.zeros_like(acc_ref)
    q = iota((1, 2 * SLOTS), 1)
    for a in range(0, peers, 2):

        @pl.when((starts[a] < stop) & (starts[a + 1] + heres[a + 1] > done))
        def _():
            row = jnp.where(q < SLOTS, q + starts[a], q - SLOTS + starts[a + 1])
            ends = jnp.where(q < SLOTS, starts[a] + heres[a], starts[a + 1] + heres[a + 1])
            good = (row < ends) & (row >= done) & (row < stop)
            target = jnp.where(good, row - done, -1)
            base = pl.multiple_of(jnp.maximum(starts[a] - done, 0) // 16 * 16, 16)
            one = jnp.where(iota((2 * SLOTS, 1), 0) + base == target, 1.0, 0.0).astype(BF16)
            pair = jnp.concatenate([blocks[a][...], blocks[a + 1][...]], axis=0)
            rows = jnp.dot(one, pair, preferred_element_type=F32)
            window = pl.ds(pl.multiple_of(base + head, 16), 2 * SLOTS)
            dense_ref[window, :] = (dense_ref[window, :].astype(F32) + rows).astype(BF16)

    there = jnp.int32(0)
    if last:
        q = iota((1, peers * CAP_CHOSEN), 1)
        target = jnp.full((1, peers * CAP_CHOSEN), -1, I32)
        for a in range(peers):
            here = jnp.clip(counts_ref[1, sources[a]] - turn * CAP_CHOSEN, 0, CAP_CHOSEN)
            slot = q - a * CAP_CHOSEN
            target = jnp.where((slot >= 0) & (slot < here), slot + there, target)
            there = there + here
        one = jnp.where(iota((head, 1), 0) == target, 1.0, 0.0).astype(BF16)
        rows = jnp.concatenate([block[CAP:SLOTS, :] for block in blocks], axis=0)
        dense_ref[0:head, :] = jnp.dot(one, rows, preferred_element_type=F32).astype(BF16)

    sub = 256
    per = chunk // LANES
    low = jnp.where(iota((max(head, 8), 1), 0) < there, 0.0, -jnp.inf)

    def add_up(i, first, size, with_head):
        lines = pl.ds(pl.multiple_of(i * per, per), per)
        level = best_ref[lines, :]
        scaled = level * (1.0 / scale)
        for u in range(chunk // sub):
            sims = lax.dot_general(dense_ref[pl.ds(first, size), :], tall_ref[i, pl.ds(u * sub, sub), :],
                                   (((1,), (1,)), ((), ())), preferred_element_type=F32)
            skip = head if with_head else 0
            part = acc_ref[pl.ds(first + skip, size - skip), :]
            for j in range(sub // LANES):
                k = u * (sub // LANES) + j
                cols = sims[:, j * LANES : (j + 1) * LANES]
                part += jnp.maximum(cols[skip:] - scaled[k : k + 1, :], 0.0)
                if with_head:
                    top = jnp.max(cols[:skip] + low, axis=0, keepdims=True) * scale
                    level_ref[pl.ds(i * per + k, 1), :] = jnp.maximum(level[k : k + 1, :], top)
            acc_ref[pl.ds(first + skip, size - skip), :] = part

    def main_step(i, carry):
        pltpu.make_async_copy(slab_ref.at[pl.ds(0, chunk), :], tall_ref.at[i], sems.at[i]).wait()
        add_up(i, 0, head + main, last)
        return carry

    lax.fori_loop(0, chunks, main_step, 0)

    slab = lax.shift_right_arithmetic(cand_ref[...], shift)
    slot = rank_ref[...] - turn * CAP
    place = jnp.full(slot.shape, -1, I32)
    for a in range(peers):
        place = jnp.where(slab == sources[a], slot + starts[a] - done, place)
    good = (slot >= 0) & (slot < CAP) & (place >= 0) & (place < stop - done)
    place = jnp.where(good, place, -1)

    def hand_out(ref, first, size):
        sums = jnp.sum(acc_ref[pl.ds(head + first, size), :], axis=1, keepdims=True) * scale
        at = iota((size, LANES), 0) + first
        for j in range(slot.shape[0]):
            mine = jnp.where(at == place[j : j + 1, :], sums, 0.0)
            out_ref[j : j + 1, :] = ref[j : j + 1, :] + jnp.sum(mine, axis=0, keepdims=True)

    hand_out(before_ref, 0, main)
    if last and total > main:

        @pl.when(stop - done > main)
        def _():
            def rest_step(i, carry):
                add_up(i, head + main, total - main, False)
                return carry

            lax.fori_loop(0, chunks, rest_step, 0)
            hand_out(out_ref, main, total - main)


def gain(turn, counts, cand, rank, before, best, slab, blocks, earlier, main, chosen, scale):
    count, width = slab.shape
    total = cand.shape[0] * cand.shape[1]
    peers = len(blocks)
    last = chosen > 0
    chunk = min(1024, count)
    body = lambda *refs: gain_kernel(*refs, peers=peers, earlier=earlier, main=main, last=last, scale=scale)
    vmem = pl.BlockSpec(memory_space=pltpu.VMEM)
    outs = [jax.ShapeDtypeStruct(cand.shape, F32)] + [jax.ShapeDtypeStruct(best.shape, F32)] * last
    rows = chosen + (total if last else main)
    made = pl.pallas_call(
        body,
        in_specs=[pl.BlockSpec(memory_space=pltpu.SMEM)] * 2 + [vmem] * 4
        + [pl.BlockSpec(memory_space=pl.ANY)] + [vmem] * peers,
        out_specs=[vmem] * len(outs),
        out_shape=outs,
        scratch_shapes=[pltpu.VMEM((rows + 2 * SLOTS, width), BF16),
                        pltpu.VMEM((rows, LANES), F32),
                        pltpu.SMEM((8,), I32),
                        pltpu.VMEM((count // chunk, chunk, width), BF16),
                        pltpu.SemaphoreType.DMA((count // chunk,))],
        compiler_params=pltpu.CompilerParams(vmem_limit_bytes=40 * 2**20),
        cost_estimate=pl.CostEstimate(flops=2 * count * width * (main + chosen), transcendentals=0,
                                      bytes_accessed=2 * count * width),
        name="gain_last" if last else "gain",
    )(turn, counts, cand, rank, before, best, slab, *blocks)
    return made if last else made[0]


def device(x, y, c):
    return (x % 4) * 4 + y * 2 + c


def moved(array, dx, dy, dc):
    pairs = [(device(x, y, c), device(x + (dx if c == 0 else -dx), y ^ dy, c ^ dc))
             for x in range(4) for y in range(2) for c in range(2)]
    return lax.ppermute(array, "ground", pairs)


def arrivals():
    me = lax.axis_index("ground")
    x, y, c = me // 4, me // 2 % 2, me % 2
    sign = 1 - 2 * c
    near = [(0, y), (0, 1 - y), (-sign, y), (sign, y)]
    far = [(2, y), (-sign, 1 - y), (sign, 1 - y), (2, 1 - y)]
    here = lambda places: [(x + dx + 4) % 4 * 4 + yy * 2 + c for dx, yy in places]
    there = lambda places: [(x - dx + 4) % 4 * 4 + yy * 2 + 1 - c for dx, yy in places]
    return here(near) + there(near) + here(far) + there(far)


def near_blocks(own):
    flip = moved(own, 0, 1, 0)
    ahead = moved(own, 1, 0, 0)
    behind = moved(own, -1, 0, 0)
    return both_cores([own, flip, ahead, behind])


def far_blocks(near):
    own, flip, ahead, behind = near[:4]
    across = moved(ahead, 1, 0, 0)
    flip_ahead = moved(flip, 1, 0, 0)
    flip_behind = moved(flip, -1, 0, 0)
    flip_across = moved(across, 0, 1, 0)
    return [across, flip_ahead, flip_behind, flip_across]


def both_cores(mine):
    return mine + [moved(block, 0, 0, 1) for block in mine]


def body(ground_rows, best, cand_index, chosen_index):
    count, width = ground_rows.shape
    scale = width ** (-0.5)
    peers = lax.axis_size("ground")
    whole = count * peers
    cand = cand_index.reshape(-1, LANES)
    chosen = chosen_index.reshape(1, -1)
    level = best.reshape(-1, LANES)
    total = cand_index.shape[0]
    first_rows = total * 13 // 32

    def finish(turn, limit, counts, rank, gains, level, blocks):
        state = jnp.stack([turn, limit]).astype(I32)
        return gain(state, counts, cand, rank, gains, level, ground_rows, blocks, peers // 2,
                    total - first_rows, chosen.shape[1], scale)

    block, rank, counts = pick(jnp.zeros((1,), I32), cand, chosen, ground_rows)
    near = near_blocks(block)
    far = far_blocks(near)
    gains = gain(jnp.zeros((2,), I32), counts, cand, rank, jnp.zeros(cand.shape, F32), level, ground_rows, near,
                 0, first_rows, 0, scale)
    gains, far = lax.optimization_barrier((gains, far))
    far = both_cores(far)
    gains, new = finish(jnp.int32(0), jnp.int32(first_rows), counts, rank, gains, level, near + far)
    turns = counts[2, 0]

    def more(state):
        return state[0] < turns

    def again(state):
        turn, gains, new = state
        block, rank, counts = pick(turn.reshape(1), cand, chosen, ground_rows)
        near = near_blocks(block)
        added, raised = finish(turn, jnp.int32(0), counts, rank, gains, level, near + both_cores(far_blocks(near)))
        return turn + 1, added, jnp.maximum(new, raised)

    unused, gains, new = lax.while_loop(more, again, (jnp.int32(1), gains, new))
    blocks = gains.reshape(peers, -1) / whole
    arrived = lax.all_to_all(blocks, "ground", 0, 0, tiled=True)
    return arrived.sum(axis=0), new.reshape(-1)


def solution(mesh):
    in_specs = (P("ground", None), P("ground"), P("cand"), P())
    out_specs = (P(("cand", "ground")), P("ground"))
    return jax.shard_map(body, mesh=mesh, in_specs=in_specs, out_specs=out_specs, check_vma=False)
```

```python
import jax
import jax.numpy as jnp
from jax import lax
from jax.experimental import pallas as pl
from jax.experimental.pallas import tpu as pltpu
from jax.sharding import PartitionSpec as P

CAP = 96
CAP_CHOSEN = 16
SLOTS = CAP + CAP_CHOSEN
LANES = 128
TILE = 8

F32 = jnp.float32
BF16 = jnp.bfloat16
I32 = jnp.int32


def iota(shape, dim):
    return lax.broadcasted_iota(I32, shape, dim)


def pick_kernel(turn_ref, cand_ref, chosen_ref, slab_ref, block_ref, rank_ref, counts_ref,
                pad_ref, list_ref, slots_ref, stage_ref, sem, list_sem):
    count = slab_ref.shape[0]
    shift = count.bit_length() - 1
    me = lax.axis_index("ground")
    turn = turn_ref[0]
    rows = cand_ref.shape[0]
    lane = iota((LANES, LANES), 1)
    line = iota((LANES, LANES), 0)
    upper = jnp.where(line <= lane, 1.0, 0.0).astype(BF16)

    pad_ref[...] = jnp.full(pad_ref.shape, -1, I32)
    pad_ref[0:1, 0 : chosen_ref.shape[1]] = chosen_ref[...]
    index = jnp.concatenate([cand_ref[...], pad_ref[...]], axis=0)
    mine = lax.shift_right_arithmetic(index, shift) == me
    upto = jnp.dot(jnp.where(mine, 1.0, 0.0).astype(BF16), upper, preferred_element_type=F32)
    ends = jnp.broadcast_to(upto[:, LANES - 1 : LANES], upto.shape)
    before = jnp.zeros((1, LANES), F32)
    lines = []
    for j in range(rows):
        lines.append(before)
        before = before + ends[j : j + 1, :]
    ahead = jnp.concatenate(lines + [jnp.zeros((8, LANES), F32)], axis=0)
    slot = (upto - 1.0 + ahead).astype(I32)
    top = iota(index.shape, 0) < rows
    slot = slot - turn * jnp.where(top, CAP, CAP_CHOSEN)
    inside = mine & (slot >= 0) & (slot < jnp.where(top, CAP, CAP_CHOSEN))
    slot = jnp.where(inside, jnp.where(top, slot, slot + CAP), -1)
    packed = jnp.where(inside, index - me * count, 0)
    slot_t = slot.T
    packed_t = packed.T
    found = jnp.zeros((LANES, LANES), I32)
    for j in range(rows + 1):
        found += jnp.where(slot_t[:, j : j + 1] == lane, packed_t[:, j : j + 1], 0)
    row = jnp.sum(found.astype(F32), axis=0, keepdims=True)
    row = jnp.broadcast_to(row, (8, LANES))
    list_ref[...] = row.astype(I32)
    copy = pltpu.make_async_copy(list_ref, slots_ref, list_sem)
    copy.start()
    copy.wait()
    for p in range(SLOTS):
        tile = lax.shift_right_logical(slots_ref[0, p], 3)
        pltpu.make_async_copy(slab_ref.at[pl.ds(pl.multiple_of(tile * TILE, TILE), TILE), :],
                              stage_ref.at[pl.ds(p * TILE, TILE), :], sem).start()

    lower = jnp.where(line >= lane, 1.0, 0.0).astype(BF16)
    index_t = index.T

    def ranked(col, carry):
        hot = lax.shift_right_arithmetic(col, shift) == lane
        upto = jnp.dot(lower, jnp.where(hot, 1.0, 0.0).astype(BF16), preferred_element_type=F32)
        rank = jnp.sum(jnp.where(hot, upto - 1.0 + carry, 0.0), axis=1, keepdims=True)
        return rank, carry + upto[LANES - 1 : LANES, :]

    counts = jnp.zeros((1, LANES), F32)
    ranks = []
    for j in range(rows):
        rank, counts = ranked(index_t[:, j : j + 1], counts)
        ranks.append(rank)
    rank_ref[...] = jnp.concatenate(ranks, axis=1).T.astype(I32)
    unused, ccounts = ranked(index_t[:, rows : rows + 1], jnp.zeros((1, LANES), F32))
    turns = jnp.maximum(
        (jnp.max(counts, axis=1, keepdims=True).astype(I32) + CAP - 1) // CAP,
        (jnp.max(ccounts, axis=1, keepdims=True).astype(I32) + CAP_CHOSEN - 1) // CAP_CHOSEN,
    )
    counts_ref[0:1, :] = counts.astype(I32)
    counts_ref[1:2, :] = ccounts.astype(I32)
    counts_ref[2:3, :] = jnp.broadcast_to(turns, (1, LANES))

    inner = row.T[:, 0:1].astype(I32) & (TILE - 1)
    want = inner[:SLOTS] + TILE * iota((SLOTS, 1), 0)
    one = jnp.where(iota((SLOTS, SLOTS * TILE), 1) == want, 1.0, 0.0).astype(BF16)
    pltpu.make_async_copy(slab_ref.at[pl.ds(0, SLOTS * TILE), :], stage_ref, sem).wait()
    block_ref[...] = jnp.dot(one, stage_ref[...], preferred_element_type=F32).astype(BF16)


def pick(turn, cand, chosen, slab):
    width = slab.shape[1]
    return pl.pallas_call(
        pick_kernel,
        in_specs=[pl.BlockSpec(memory_space=pltpu.SMEM), pl.BlockSpec(memory_space=pltpu.VMEM),
                  pl.BlockSpec(memory_space=pltpu.VMEM), pl.BlockSpec(memory_space=pl.ANY)],
        out_specs=[pl.BlockSpec(memory_space=pltpu.VMEM)] * 3,
        out_shape=[pltpu.VMEM((SLOTS, width), BF16), pltpu.VMEM(cand.shape, I32), pltpu.VMEM((8, LANES), I32)],
        scratch_shapes=[pltpu.VMEM((8, LANES), I32), pltpu.VMEM((8, LANES), I32),
                        pltpu.SMEM((8, LANES), I32), pltpu.VMEM((SLOTS * TILE, width), BF16),
                        pltpu.SemaphoreType.DMA, pltpu.SemaphoreType.DMA],
        name="pick",
    )(turn, cand, chosen, slab)


def gain_kernel(turn_ref, counts_ref, cand_ref, rank_ref, before_ref, best_ref, slab_ref, *rest,
                peers, earlier, main, last, scale):
    blocks = rest[:peers]
    if last:
        out_ref, level_ref, dense_ref, acc_ref, at_ref, tall_ref, sems = rest[peers:]
    else:
        out_ref, dense_ref, acc_ref, at_ref, tall_ref, sems = rest[peers:]
        level_ref = None
    chunks, chunk, width = tall_ref.shape
    count = slab_ref.shape[0]
    shift = count.bit_length() - 1
    total = cand_ref.shape[0] * cand_ref.shape[1]
    head = dense_ref.shape[0] - 2 * SLOTS - (total if last else main)
    turn = turn_ref[0]
    for i in range(chunks):
        pltpu.make_async_copy(slab_ref.at[pl.ds(i * chunk, chunk), :], tall_ref.at[i], sems.at[i]).start()

    sources = arrivals()[:peers]
    start = jnp.int32(0)
    done = jnp.int32(0)
    starts, heres = [], []
    for a in range(peers):
        if a == earlier:
            done = jnp.minimum(start, turn_ref[1])
        here = jnp.clip(counts_ref[0, sources[a]] - turn * CAP, 0, CAP)
        starts.append(start)
        heres.append(here)
        start = start + here
    stop = start if last else jnp.minimum(start, main)

    dense_ref[...] = jnp.zeros_like(dense_ref)
    acc_ref[...] = jnp.zeros_like(acc_ref)
    q = iota((1, 2 * SLOTS), 1)
    for a in range(0, peers, 2):

        @pl.when((starts[a] < stop) & (starts[a + 1] + heres[a + 1] > done))
        def _():
            row = jnp.where(q < SLOTS, q + starts[a], q - SLOTS + starts[a + 1])
            ends = jnp.where(q < SLOTS, starts[a] + heres[a], starts[a + 1] + heres[a + 1])
            good = (row < ends) & (row >= done) & (row < stop)
            target = jnp.where(good, row - done, -1)
            base = pl.multiple_of(jnp.maximum(starts[a] - done, 0) // 16 * 16, 16)
            one = jnp.where(iota((2 * SLOTS, 1), 0) + base == target, 1.0, 0.0).astype(BF16)
            pair = jnp.concatenate([blocks[a][...], blocks[a + 1][...]], axis=0)
            rows = jnp.dot(one, pair, preferred_element_type=F32)
            window = pl.ds(pl.multiple_of(base + head, 16), 2 * SLOTS)
            dense_ref[window, :] = (dense_ref[window, :].astype(F32) + rows).astype(BF16)

    there = jnp.int32(0)
    if last:
        q = iota((1, peers * CAP_CHOSEN), 1)
        target = jnp.full((1, peers * CAP_CHOSEN), -1, I32)
        for a in range(peers):
            here = jnp.clip(counts_ref[1, sources[a]] - turn * CAP_CHOSEN, 0, CAP_CHOSEN)
            slot = q - a * CAP_CHOSEN
            target = jnp.where((slot >= 0) & (slot < here), slot + there, target)
            there = there + here
        one = jnp.where(iota((head, 1), 0) == target, 1.0, 0.0).astype(BF16)
        rows = jnp.concatenate([block[CAP:SLOTS, :] for block in blocks], axis=0)
        dense_ref[0:head, :] = jnp.dot(one, rows, preferred_element_type=F32).astype(BF16)

    sub = 256
    per = chunk // LANES
    low = jnp.where(iota((max(head, 8), 1), 0) < there, 0.0, -jnp.inf)

    def add_up(i, first, size, with_head, tiles):
        lines = pl.ds(pl.multiple_of(i * per, per), per)
        level = best_ref[lines, :]
        scaled = level * (1.0 / scale)
        for u in tiles:
            sims = lax.dot_general(dense_ref[pl.ds(first, size), :], tall_ref[i, pl.ds(u * sub, sub), :],
                                   (((1,), (1,)), ((), ())), preferred_element_type=F32)
            skip = head if with_head else 0
            part = acc_ref[pl.ds(first + skip, size - skip), :]
            for j in range(sub // LANES):
                k = u * (sub // LANES) + j
                cols = sims[:, j * LANES : (j + 1) * LANES]
                part += jnp.maximum(cols[skip:] - scaled[k : k + 1, :], 0.0)
                if with_head:
                    top = jnp.max(cols[:skip] + low, axis=0, keepdims=True) * scale
                    level_ref[pl.ds(i * per + k, 1), :] = jnp.maximum(level[k : k + 1, :], top)
            acc_ref[pl.ds(first + skip, size - skip), :] = part

    def main_step(i, carry):
        pltpu.make_async_copy(slab_ref.at[pl.ds(0, chunk), :], tall_ref.at[i], sems.at[i]).wait()
        add_up(i, 0, head + main, last, range(chunk // sub))
        return carry

    lax.fori_loop(0, chunks, main_step, 0)

    slab = lax.shift_right_arithmetic(cand_ref[...], shift)
    slot = rank_ref[...] - turn * CAP
    place = jnp.full(slot.shape, -1, I32)
    for a in range(peers):
        place = jnp.where(slab == sources[a], slot + starts[a] - done, place)
    good = (slot >= 0) & (slot < CAP) & (place >= 0) & (place < stop - done)
    place = jnp.where(good, place, -1)

    def hand_out(ref, first, size):
        sums = jnp.sum(acc_ref[pl.ds(head + first, size), :], axis=1, keepdims=True) * scale
        at = iota((size, LANES), 0) + first
        for j in range(slot.shape[0]):
            mine = jnp.where(at == place[j : j + 1, :], sums, 0.0)
            out_ref[j : j + 1, :] = ref[j : j + 1, :] + jnp.sum(mine, axis=0, keepdims=True)

    hand_out(before_ref, 0, main)
    if last and total > main:

        @pl.when(stop - done > main)
        def _():
            def rest_step(k, carry):
                lines = sub // LANES
                edges = best_ref[pl.ds(k * lines, lines), :] * (1.0 / scale)
                i, u = k // (chunk // sub), k % (chunk // sub)
                tall = tall_ref[i, pl.ds(pl.multiple_of(u * sub, sub), sub), :]
                sims = lax.dot_general(dense_ref[pl.ds(head + main, total - main), :], tall,
                                       (((1,), (1,)), ((), ())), preferred_element_type=F32)
                for j in range(lines):
                    cols = sims[:, j * LANES : (j + 1) * LANES]
                    acc_ref[pl.ds(head + main, total - main), :] += jnp.maximum(cols - edges[j : j + 1, :], 0.0)
                return carry

            lax.fori_loop(0, chunks * (chunk // sub), rest_step, 0)
            hand_out(out_ref, main, total - main)


def gain(turn, counts, cand, rank, before, best, slab, blocks, earlier, main, chosen, scale):
    count, width = slab.shape
    total = cand.shape[0] * cand.shape[1]
    peers = len(blocks)
    last = chosen > 0
    chunk = min(2048, count)
    body = lambda *refs: gain_kernel(*refs, peers=peers, earlier=earlier, main=main, last=last, scale=scale)
    vmem = pl.BlockSpec(memory_space=pltpu.VMEM)
    outs = [jax.ShapeDtypeStruct(cand.shape, F32)] + [jax.ShapeDtypeStruct(best.shape, F32)] * last
    rows = chosen + (total if last else main)
    made = pl.pallas_call(
        body,
        in_specs=[pl.BlockSpec(memory_space=pltpu.SMEM)] * 2 + [vmem] * 4
        + [pl.BlockSpec(memory_space=pl.ANY)] + [vmem] * peers,
        out_specs=[vmem] * len(outs),
        out_shape=outs,
        scratch_shapes=[pltpu.VMEM((rows + 2 * SLOTS, width), BF16),
                        pltpu.VMEM((rows, LANES), F32),
                        pltpu.SMEM((8,), I32),
                        pltpu.VMEM((count // chunk, chunk, width), BF16),
                        pltpu.SemaphoreType.DMA((count // chunk,))],
        compiler_params=pltpu.CompilerParams(vmem_limit_bytes=40 * 2**20),
        cost_estimate=pl.CostEstimate(flops=2 * count * width * (main + chosen), transcendentals=0,
                                      bytes_accessed=2 * count * width),
        name="gain_last" if last else "gain",
    )(turn, counts, cand, rank, before, best, slab, *blocks)
    return made if last else made[0]


def device(x, y, c):
    return (x % 4) * 4 + y * 2 + c


def moved(array, dx, dy, dc):
    pairs = [(device(x, y, c), device(x + (dx if c == 0 else -dx), y ^ dy, c ^ dc))
             for x in range(4) for y in range(2) for c in range(2)]
    return lax.ppermute(array, "ground", pairs)


def arrivals():
    me = lax.axis_index("ground")
    x, y, c = me // 4, me // 2 % 2, me % 2
    sign = 1 - 2 * c
    near = [(0, y), (0, 1 - y), (-sign, y), (sign, y)]
    far = [(2, y), (-sign, 1 - y), (sign, 1 - y), (2, 1 - y)]
    here = lambda places: [(x + dx + 4) % 4 * 4 + yy * 2 + c for dx, yy in places]
    there = lambda places: [(x - dx + 4) % 4 * 4 + yy * 2 + 1 - c for dx, yy in places]
    return here(near) + there(near) + here(far) + there(far)


def near_blocks(own):
    flip = moved(own, 0, 1, 0)
    ahead = moved(own, 1, 0, 0)
    behind = moved(own, -1, 0, 0)
    return both_cores([own, flip, ahead, behind])


def far_blocks(near):
    own, flip, ahead, behind = near[:4]
    across = moved(ahead, 1, 0, 0)
    flip_ahead = moved(flip, 1, 0, 0)
    flip_behind = moved(flip, -1, 0, 0)
    flip_across = moved(ahead, 1, 1, 0)
    return [across, flip_ahead, flip_behind, flip_across]


def both_cores(mine):
    return mine + [moved(block, 0, 0, 1) for block in mine]


def body(ground_rows, best, cand_index, chosen_index):
    count, width = ground_rows.shape
    scale = width ** (-0.5)
    peers = lax.axis_size("ground")
    whole = count * peers
    cand = cand_index.reshape(-1, LANES)
    chosen = chosen_index.reshape(1, -1)
    level = best.reshape(-1, LANES)
    total = cand_index.shape[0]
    first_rows = total * 13 // 32

    def finish(turn, limit, counts, rank, gains, level, blocks):
        state = jnp.stack([turn, limit]).astype(I32)
        return gain(state, counts, cand, rank, gains, level, ground_rows, blocks, peers // 2,
                    total - first_rows, chosen.shape[1], scale)

    block, rank, counts = pick(jnp.zeros((1,), I32), cand, chosen, ground_rows)
    near = near_blocks(block)
    far = far_blocks(near)
    gains = gain(jnp.zeros((2,), I32), counts, cand, rank, jnp.zeros(cand.shape, F32), level, ground_rows, near,
                 0, first_rows, 0, scale)
    gains, far = lax.optimization_barrier((gains, far))
    far = both_cores(far)
    gains, new = finish(jnp.int32(0), jnp.int32(first_rows), counts, rank, gains, level, near + far)
    turns = counts[2, 0]

    def more(state):
        return state[0] < turns

    def again(state):
        turn, gains, new = state
        block, rank, counts = pick(turn.reshape(1), cand, chosen, ground_rows)
        near = near_blocks(block)
        added, raised = finish(turn, jnp.int32(0), counts, rank, gains, level, near + both_cores(far_blocks(near)))
        return turn + 1, added, jnp.maximum(new, raised)

    unused, gains, new = lax.while_loop(more, again, (jnp.int32(1), gains, new))
    blocks = gains.reshape(peers, -1) / whole
    arrived = lax.all_to_all(blocks, "ground", 0, 0, tiled=True)
    return arrived.sum(axis=0), new.reshape(-1)


def solution(mesh):
    in_specs = (P("ground", None), P("ground"), P("cand"), P())
    out_specs = (P(("cand", "ground")), P("ground"))
    return jax.shard_map(body, mesh=mesh, in_specs=in_specs, out_specs=out_specs, check_vma=False)
```

```python
import jax
import jax.numpy as jnp
from jax import lax
from jax.experimental import pallas as pl
from jax.experimental.pallas import tpu as pltpu
from jax.sharding import PartitionSpec as P


CAP = 96
CAP_CHOSEN = 16
SLOTS = CAP + CAP_CHOSEN
LANES = 128
TILE = 8

F32 = jnp.float32
BF16 = jnp.bfloat16
I32 = jnp.int32


def iota(shape, dim):
    return lax.broadcasted_iota(I32, shape, dim)


def pick_kernel(turn_ref, cand_ref, chosen_ref, slab_ref, block_ref, rank_ref, counts_ref,
                pad_ref, list_ref, slots_ref, stage_ref, sem, list_sem):
    count = slab_ref.shape[0]
    shift = count.bit_length() - 1
    me = lax.axis_index("ground")
    turn = turn_ref[0]
    rows = cand_ref.shape[0]
    lane = iota((LANES, LANES), 1)
    line = iota((LANES, LANES), 0)
    upper = jnp.where(line <= lane, 1.0, 0.0).astype(BF16)

    pad_ref[...] = jnp.full(pad_ref.shape, -1, I32)
    pad_ref[0:1, 0 : chosen_ref.shape[1]] = chosen_ref[...]
    index = jnp.concatenate([cand_ref[...], pad_ref[...]], axis=0)
    mine = lax.shift_right_arithmetic(index, shift) == me
    upto = jnp.dot(jnp.where(mine, 1.0, 0.0).astype(BF16), upper, preferred_element_type=F32)
    ends = jnp.broadcast_to(upto[:, LANES - 1 : LANES], upto.shape)
    before = jnp.zeros((1, LANES), F32)
    lines = []
    for j in range(rows):
        lines.append(before)
        before = before + ends[j : j + 1, :]
    ahead = jnp.concatenate(lines + [jnp.zeros((8, LANES), F32)], axis=0)
    slot = (upto - 1.0 + ahead).astype(I32)
    top = iota(index.shape, 0) < rows
    slot = slot - turn * jnp.where(top, CAP, CAP_CHOSEN)
    inside = mine & (slot >= 0) & (slot < jnp.where(top, CAP, CAP_CHOSEN))
    slot = jnp.where(inside, jnp.where(top, slot, slot + CAP), -1)
    packed = jnp.where(inside, index - me * count, 0)
    slot_t = slot.T
    packed_t = packed.T
    found = jnp.zeros((LANES, LANES), I32)
    for j in range(rows + 1):
        found += jnp.where(slot_t[:, j : j + 1] == lane, packed_t[:, j : j + 1], 0)
    row = jnp.sum(found.astype(F32), axis=0, keepdims=True)
    row = jnp.broadcast_to(row, (8, LANES))
    list_ref[...] = row.astype(I32)
    copy = pltpu.make_async_copy(list_ref, slots_ref, list_sem)
    copy.start()
    copy.wait()
    for p in range(SLOTS):
        tile = lax.shift_right_logical(slots_ref[0, p], 3)
        pltpu.make_async_copy(slab_ref.at[pl.ds(pl.multiple_of(tile * TILE, TILE), TILE), :],
                              stage_ref.at[pl.ds(p * TILE, TILE), :], sem).start()

    lower = jnp.where(line >= lane, 1.0, 0.0).astype(BF16)
    index_t = index.T

    def ranked(col, carry):
        hot = lax.shift_right_arithmetic(col, shift) == lane
        upto = jnp.dot(lower, jnp.where(hot, 1.0, 0.0).astype(BF16), preferred_element_type=F32)
        rank = jnp.sum(jnp.where(hot, upto - 1.0 + carry, 0.0), axis=1, keepdims=True)
        return rank, carry + upto[LANES - 1 : LANES, :]

    counts = jnp.zeros((1, LANES), F32)
    ranks = []
    for j in range(rows):
        rank, counts = ranked(index_t[:, j : j + 1], counts)
        ranks.append(rank)
    rank_ref[...] = jnp.concatenate(ranks, axis=1).T.astype(I32)
    _, ccounts = ranked(index_t[:, rows : rows + 1], jnp.zeros((1, LANES), F32))
    turns = jnp.maximum(
        (jnp.max(counts, axis=1, keepdims=True).astype(I32) + CAP - 1) // CAP,
        (jnp.max(ccounts, axis=1, keepdims=True).astype(I32) + CAP_CHOSEN - 1) // CAP_CHOSEN,
    )
    counts_ref[0:1, :] = counts.astype(I32)
    counts_ref[1:2, :] = ccounts.astype(I32)
    counts_ref[2:3, :] = jnp.broadcast_to(turns, (1, LANES))

    inner = row.T[:, 0:1].astype(I32) & (TILE - 1)
    want = inner[:SLOTS] + TILE * iota((SLOTS, 1), 0)
    one = jnp.where(iota((SLOTS, SLOTS * TILE), 1) == want, 1.0, 0.0).astype(BF16)
    pltpu.make_async_copy(slab_ref.at[pl.ds(0, SLOTS * TILE), :], stage_ref, sem).wait()
    block_ref[...] = jnp.dot(one, stage_ref[...], preferred_element_type=F32).astype(BF16)


def pick(turn, cand, chosen, slab):
    width = slab.shape[1]
    return pl.pallas_call(
        pick_kernel,
        in_specs=[pl.BlockSpec(memory_space=pltpu.SMEM), pl.BlockSpec(memory_space=pltpu.VMEM),
                  pl.BlockSpec(memory_space=pltpu.VMEM), pl.BlockSpec(memory_space=pl.ANY)],
        out_specs=[pl.BlockSpec(memory_space=pltpu.VMEM)] * 3,
        out_shape=[pltpu.VMEM((SLOTS, width), BF16), pltpu.VMEM(cand.shape, I32), pltpu.VMEM((8, LANES), I32)],
        scratch_shapes=[pltpu.VMEM((8, LANES), I32), pltpu.VMEM((8, LANES), I32),
                        pltpu.SMEM((8, LANES), I32), pltpu.VMEM((SLOTS * TILE, width), BF16),
                        pltpu.SemaphoreType.DMA, pltpu.SemaphoreType.DMA],
        name="pick",
    )(turn, cand, chosen, slab)


def gain_kernel(turn_ref, counts_ref, cand_ref, rank_ref, before_ref, best_ref, slab_ref, *rest,
                peers, earlier, main, last, scale):
    blocks = rest[:peers]
    if last:
        out_ref, level_ref, dense_ref, acc_ref, at_ref, tall_ref, sems = rest[peers:]
    else:
        out_ref, dense_ref, acc_ref, at_ref, tall_ref, sems = rest[peers:]
        level_ref = None
    chunks, chunk, _ = tall_ref.shape
    count = slab_ref.shape[0]
    shift = count.bit_length() - 1
    total = cand_ref.shape[0] * cand_ref.shape[1]
    head = dense_ref.shape[0] - 2 * SLOTS - (total if last else main)
    turn = turn_ref[0]
    for i in range(chunks):
        pltpu.make_async_copy(slab_ref.at[pl.ds(i * chunk, chunk), :], tall_ref.at[i], sems.at[i]).start()

    sources = arrivals()[:peers]
    start = jnp.int32(0)
    done = jnp.int32(0)
    starts, heres = [], []
    for a in range(peers):
        if a == earlier:
            done = jnp.minimum(start, turn_ref[1])
        here = jnp.clip(counts_ref[0, sources[a]] - turn * CAP, 0, CAP)
        starts.append(start)
        heres.append(here)
        start = start + here
    stop = start if last else jnp.minimum(start, main)

    dense_ref[...] = jnp.zeros_like(dense_ref)
    acc_ref[...] = jnp.zeros_like(acc_ref)
    q = iota((1, 2 * SLOTS), 1)
    for a in range(0, peers, 2):

        @pl.when((starts[a] < stop) & (starts[a + 1] + heres[a + 1] > done))
        def _():
            row = jnp.where(q < SLOTS, q + starts[a], q - SLOTS + starts[a + 1])
            ends = jnp.where(q < SLOTS, starts[a] + heres[a], starts[a + 1] + heres[a + 1])
            good = (row < ends) & (row >= done) & (row < stop)
            target = jnp.where(good, row - done, -1)
            base = pl.multiple_of(jnp.maximum(starts[a] - done, 0) // 16 * 16, 16)
            one = jnp.where(iota((2 * SLOTS, 1), 0) + base == target, 1.0, 0.0).astype(BF16)
            pair = jnp.concatenate([blocks[a][...], blocks[a + 1][...]], axis=0)
            rows = jnp.dot(one, pair, preferred_element_type=F32)
            window = pl.ds(pl.multiple_of(base + head, 16), 2 * SLOTS)
            dense_ref[window, :] = (dense_ref[window, :].astype(F32) + rows).astype(BF16)

    there = jnp.int32(0)
    if last:
        q = iota((1, peers * CAP_CHOSEN), 1)
        target = jnp.full((1, peers * CAP_CHOSEN), -1, I32)
        for a in range(peers):
            here = jnp.clip(counts_ref[1, sources[a]] - turn * CAP_CHOSEN, 0, CAP_CHOSEN)
            slot = q - a * CAP_CHOSEN
            target = jnp.where((slot >= 0) & (slot < here), slot + there, target)
            there = there + here
        one = jnp.where(iota((head, 1), 0) == target, 1.0, 0.0).astype(BF16)
        rows = jnp.concatenate([block[CAP:SLOTS, :] for block in blocks], axis=0)
        dense_ref[0:head, :] = jnp.dot(one, rows, preferred_element_type=F32).astype(BF16)

    sub = 256
    per = chunk // LANES
    low = jnp.where(iota((max(head, 8), 1), 0) < there, 0.0, -jnp.inf)

    def add_up(i, first, size, with_head, tiles):
        lines = pl.ds(pl.multiple_of(i * per, per), per)
        level = best_ref[lines, :]
        scaled = level * (1.0 / scale)
        for u in tiles:
            sims = lax.dot_general(dense_ref[pl.ds(first, size), :], tall_ref[i, pl.ds(u * sub, sub), :],
                                   (((1,), (1,)), ((), ())), preferred_element_type=F32)
            skip = head if with_head else 0
            part = acc_ref[pl.ds(first + skip, size - skip), :]
            for j in range(sub // LANES):
                k = u * (sub // LANES) + j
                cols = sims[:, j * LANES : (j + 1) * LANES]
                part += jnp.maximum(cols[skip:] - scaled[k : k + 1, :], 0.0)
                if with_head:
                    top = jnp.max(cols[:skip] + low, axis=0, keepdims=True) * scale
                    level_ref[pl.ds(i * per + k, 1), :] = jnp.maximum(level[k : k + 1, :], top)
            acc_ref[pl.ds(first + skip, size - skip), :] = part

    def main_step(i, carry):
        pltpu.make_async_copy(slab_ref.at[pl.ds(0, chunk), :], tall_ref.at[i], sems.at[i]).wait()
        add_up(i, 0, head + main, last, range(chunk // sub))
        return carry

    lax.fori_loop(0, chunks, main_step, 0)

    slab = lax.shift_right_arithmetic(cand_ref[...], shift)
    slot = rank_ref[...] - turn * CAP
    place = jnp.full(slot.shape, -1, I32)
    for a in range(peers):
        place = jnp.where(slab == sources[a], slot + starts[a] - done, place)
    good = (slot >= 0) & (slot < CAP) & (place >= 0) & (place < stop - done)
    place = jnp.where(good, place, -1)

    def hand_out(ref, first, size):
        sums = jnp.sum(acc_ref[pl.ds(head + first, size), :], axis=1, keepdims=True) * scale
        at = iota((size, LANES), 0) + first
        for j in range(slot.shape[0]):
            mine = jnp.where(at == place[j : j + 1, :], sums, 0.0)
            out_ref[j : j + 1, :] = ref[j : j + 1, :] + jnp.sum(mine, axis=0, keepdims=True)

    hand_out(before_ref, 0, main)
    if last and total > main:

        @pl.when(stop - done > main)
        def _():
            def rest_step(k, carry):
                lines = sub // LANES
                edges = best_ref[pl.ds(k * lines, lines), :] * (1.0 / scale)
                i, u = k // (chunk // sub), k % (chunk // sub)
                tall = tall_ref[i, pl.ds(pl.multiple_of(u * sub, sub), sub), :]
                sims = lax.dot_general(dense_ref[pl.ds(head + main, total - main), :], tall,
                                       (((1,), (1,)), ((), ())), preferred_element_type=F32)
                for j in range(lines):
                    cols = sims[:, j * LANES : (j + 1) * LANES]
                    acc_ref[pl.ds(head + main, total - main), :] += jnp.maximum(cols - edges[j : j + 1, :], 0.0)
                return carry

            lax.fori_loop(0, chunks * (chunk // sub), rest_step, 0)
            hand_out(out_ref, main, total - main)


def gain(turn, counts, cand, rank, before, best, slab, blocks, earlier, main, chosen, scale):
    count, width = slab.shape
    total = cand.shape[0] * cand.shape[1]
    peers = len(blocks)
    last = chosen > 0
    chunk = min(2048, count)
    body = lambda *refs: gain_kernel(*refs, peers=peers, earlier=earlier, main=main, last=last, scale=scale)
    vmem = pl.BlockSpec(memory_space=pltpu.VMEM)
    outs = [jax.ShapeDtypeStruct(cand.shape, F32)] + [jax.ShapeDtypeStruct(best.shape, F32)] * last
    rows = chosen + (total if last else main)
    made = pl.pallas_call(
        body,
        in_specs=[pl.BlockSpec(memory_space=pltpu.SMEM)] * 2 + [vmem] * 4
        + [pl.BlockSpec(memory_space=pl.ANY)] + [vmem] * peers,
        out_specs=[vmem] * len(outs),
        out_shape=outs,
        scratch_shapes=[pltpu.VMEM((rows + 2 * SLOTS, width), BF16),
                        pltpu.VMEM((rows, LANES), F32),
                        pltpu.SMEM((8,), I32),
                        pltpu.VMEM((count // chunk, chunk, width), BF16),
                        pltpu.SemaphoreType.DMA((count // chunk,))],
        compiler_params=pltpu.CompilerParams(vmem_limit_bytes=40 * 2**20),
        cost_estimate=pl.CostEstimate(flops=2 * count * width * (main + chosen), transcendentals=0,
                                      bytes_accessed=2 * count * width),
        name="gain_last" if last else "gain",
    )(turn, counts, cand, rank, before, best, slab, *blocks)
    return made if last else made[0]


def device(x, y, c):
    return (x % 4) * 4 + y * 2 + c


def moved(array, dx, dy, dc):
    pairs = [(device(x, y, c), device(x + (dx if c == 0 else -dx), y ^ dy, c ^ dc))
             for x in range(4) for y in range(2) for c in range(2)]
    return lax.ppermute(array, "ground", pairs)


def arrivals():
    me = lax.axis_index("ground")
    x, y, c = me // 4, me // 2 % 2, me % 2
    sign = 1 - 2 * c
    near = [(0, y), (0, 1 - y), (-sign, y), (sign, y)]
    far = [(2, y), (-sign, 1 - y), (sign, 1 - y), (2, 1 - y)]
    here = lambda places: [(x + dx + 4) % 4 * 4 + yy * 2 + c for dx, yy in places]
    there = lambda places: [(x - dx + 4) % 4 * 4 + yy * 2 + 1 - c for dx, yy in places]
    return here(near) + there(near) + here(far) + there(far)


def near_blocks(own):
    ahead = moved(own, 1, 0, 0)
    behind = moved(own, -1, 0, 0)
    flip = moved(own, 0, 1, 0)
    return both_cores([own, flip, ahead, behind])


def far_blocks(near):
    own, _, ahead, _ = near[:4]
    across = moved(ahead, 1, 0, 0)
    flip_ahead = moved(own, 1, 1, 0)
    flip_behind = moved(own, -1, 1, 0)
    flip_across = moved(ahead, 1, 1, 0)
    return [across, flip_ahead, flip_behind, flip_across]


def both_cores(mine):
    return mine + [moved(block, 0, 0, 1) for block in mine]


def body(ground_rows, best, cand_index, chosen_index):
    count, width = ground_rows.shape
    scale = width ** (-0.5)
    peers = lax.axis_size("ground")
    whole = count * peers
    cand = cand_index.reshape(-1, LANES)
    chosen = chosen_index.reshape(1, -1)
    level = best.reshape(-1, LANES)
    total = cand_index.shape[0]
    first_rows = total * 13 // 32

    def finish(turn, limit, counts, rank, gains, level, blocks):
        state = jnp.stack([turn, limit]).astype(I32)
        return gain(state, counts, cand, rank, gains, level, ground_rows, blocks, peers // 2,
                    total - first_rows, chosen.shape[1], scale)

    block, rank, counts = pick(jnp.zeros((1,), I32), cand, chosen, ground_rows)
    turns = counts[2, 0]
    near = near_blocks(block)
    far = far_blocks(near)
    gains = gain(jnp.zeros((2,), I32), counts, cand, rank, jnp.zeros(cand.shape, F32), level, ground_rows, near,
                 0, first_rows, 0, scale)
    gains, far = lax.optimization_barrier((gains, far))
    far = both_cores(far)
    gains, new = finish(jnp.int32(0), jnp.int32(first_rows), counts, rank, gains, level, near + far)

    def more(state):
        return state[0] < turns

    def again(state):
        turn, gains, new = state
        block, rank, counts = pick(turn.reshape(1), cand, chosen, ground_rows)
        near = near_blocks(block)
        added, raised = finish(turn, jnp.int32(0), counts, rank, gains, level, near + both_cores(far_blocks(near)))
        return turn + 1, added, jnp.maximum(new, raised)

    _, gains, new = lax.while_loop(more, again, (jnp.int32(1), gains, new))
    blocks = gains.reshape(peers, -1) / whole
    arrived = lax.all_to_all(blocks, "ground", 0, 0, tiled=True)
    return arrived.sum(axis=0), new.reshape(-1)


def solution(mesh):
    in_specs = (P("ground", None), P("ground"), P("cand"), P())
    out_specs = (P(("cand", "ground")), P("ground"))
    return jax.shard_map(body, mesh=mesh, in_specs=in_specs, out_specs=out_specs, check_vma=False)
```

```python
import jax
import jax.numpy as jnp
from jax import lax
from jax.experimental import pallas as pl
from jax.experimental.pallas import tpu as pltpu
from jax.sharding import PartitionSpec as P


CAP = 96
CAP_CHOSEN = 16
SLOTS = CAP + CAP_CHOSEN
LANES = 128
TILE = 8

F32 = jnp.float32
BF16 = jnp.bfloat16
I32 = jnp.int32


def iota(shape, dim):
    return lax.broadcasted_iota(I32, shape, dim)


def pick_kernel(turn_ref, cand_ref, chosen_ref, slab_ref, block_ref, rank_ref, counts_ref,
                pad_ref, list_ref, slots_ref, stage_ref, sem, list_sem):
    count = slab_ref.shape[0]
    shift = count.bit_length() - 1
    me = lax.axis_index("ground")
    turn = turn_ref[0]
    rows = cand_ref.shape[0]
    lane = iota((LANES, LANES), 1)
    line = iota((LANES, LANES), 0)
    upper = jnp.where(line <= lane, 1.0, 0.0).astype(BF16)

    pad_ref[...] = jnp.full(pad_ref.shape, -1, I32)
    pad_ref[0:1, 0 : chosen_ref.shape[1]] = chosen_ref[...]
    index = jnp.concatenate([cand_ref[...], pad_ref[...]], axis=0)
    mine = lax.shift_right_arithmetic(index, shift) == me
    upto = jnp.dot(jnp.where(mine, 1.0, 0.0).astype(BF16), upper, preferred_element_type=F32)
    ends = jnp.broadcast_to(upto[:, LANES - 1 : LANES], upto.shape)
    before = jnp.zeros((1, LANES), F32)
    lines = []
    for j in range(rows):
        lines.append(before)
        before = before + ends[j : j + 1, :]
    ahead = jnp.concatenate(lines + [jnp.zeros((8, LANES), F32)], axis=0)
    slot = (upto - 1.0 + ahead).astype(I32)
    top = iota(index.shape, 0) < rows
    slot = slot - turn * jnp.where(top, CAP, CAP_CHOSEN)
    inside = mine & (slot >= 0) & (slot < jnp.where(top, CAP, CAP_CHOSEN))
    slot = jnp.where(inside, jnp.where(top, slot, slot + CAP), -1)
    packed = jnp.where(inside, index - me * count, 0)
    slot_t = slot.T
    packed_t = packed.T
    found = jnp.zeros((LANES, LANES), I32)
    for j in range(rows + 1):
        found += jnp.where(slot_t[:, j : j + 1] == lane, packed_t[:, j : j + 1], 0)
    row = jnp.sum(found.astype(F32), axis=0, keepdims=True)
    row = jnp.broadcast_to(row, (8, LANES))
    list_ref[...] = row.astype(I32)
    copy = pltpu.make_async_copy(list_ref, slots_ref, list_sem)
    copy.start()
    copy.wait()
    for p in range(SLOTS):
        tile = lax.shift_right_logical(slots_ref[0, p], 3)
        pltpu.make_async_copy(slab_ref.at[pl.ds(pl.multiple_of(tile * TILE, TILE), TILE), :],
                              stage_ref.at[pl.ds(p * TILE, TILE), :], sem).start()

    lower = jnp.where(line >= lane, 1.0, 0.0).astype(BF16)
    index_t = index.T

    def ranked(col, carry):
        hot = lax.shift_right_arithmetic(col, shift) == lane
        upto = jnp.dot(lower, jnp.where(hot, 1.0, 0.0).astype(BF16), preferred_element_type=F32)
        rank = jnp.sum(jnp.where(hot, upto - 1.0 + carry, 0.0), axis=1, keepdims=True)
        return rank, carry + upto[LANES - 1 : LANES, :]

    counts = jnp.zeros((1, LANES), F32)
    ranks = []
    for j in range(rows):
        rank, counts = ranked(index_t[:, j : j + 1], counts)
        ranks.append(rank)
    rank_ref[...] = jnp.concatenate(ranks, axis=1).T.astype(I32)
    _, ccounts = ranked(index_t[:, rows : rows + 1], jnp.zeros((1, LANES), F32))
    turns = jnp.maximum(
        (jnp.max(counts, axis=1, keepdims=True).astype(I32) + CAP - 1) // CAP,
        (jnp.max(ccounts, axis=1, keepdims=True).astype(I32) + CAP_CHOSEN - 1) // CAP_CHOSEN,
    )
    counts_ref[0:1, :] = counts.astype(I32)
    counts_ref[1:2, :] = ccounts.astype(I32)
    counts_ref[2:3, :] = jnp.broadcast_to(turns, (1, LANES))

    inner = row.T[:, 0:1].astype(I32) & (TILE - 1)
    want = inner[:SLOTS] + TILE * iota((SLOTS, 1), 0)
    one = jnp.where(iota((SLOTS, SLOTS * TILE), 1) == want, 1.0, 0.0).astype(BF16)
    pltpu.make_async_copy(slab_ref.at[pl.ds(0, SLOTS * TILE), :], stage_ref, sem).wait()
    block_ref[...] = jnp.dot(one, stage_ref[...], preferred_element_type=F32).astype(BF16)


def pick(turn, cand, chosen, slab):
    width = slab.shape[1]
    return pl.pallas_call(
        pick_kernel,
        in_specs=[pl.BlockSpec(memory_space=pltpu.SMEM), pl.BlockSpec(memory_space=pltpu.VMEM),
                  pl.BlockSpec(memory_space=pltpu.VMEM), pl.BlockSpec(memory_space=pl.ANY)],
        out_specs=[pl.BlockSpec(memory_space=pltpu.VMEM)] * 3,
        out_shape=[pltpu.VMEM((SLOTS, width), BF16), pltpu.VMEM(cand.shape, I32), pltpu.VMEM((8, LANES), I32)],
        scratch_shapes=[pltpu.VMEM((8, LANES), I32), pltpu.VMEM((8, LANES), I32),
                        pltpu.SMEM((8, LANES), I32), pltpu.VMEM((SLOTS * TILE, width), BF16),
                        pltpu.SemaphoreType.DMA, pltpu.SemaphoreType.DMA],
        compiler_params=pltpu.CompilerParams(vmem_limit_bytes=16 * 2**20),
        name="pick",
    )(turn, cand, chosen, slab)


def gain_kernel(turn_ref, counts_ref, cand_ref, rank_ref, before_ref, best_ref, slab_ref, *rest,
                peers, earlier, main, last, scale):
    pairs = rest[: peers // 2]
    rest = rest[peers // 2 :]
    if last:
        out_ref, level_ref, dense_ref, acc_ref = rest
    else:
        out_ref, dense_ref, acc_ref = rest
        level_ref = None
    count, _ = slab_ref.shape
    chunk = min(2048, count)
    chunks = count // chunk
    shift = count.bit_length() - 1
    total = cand_ref.shape[0] * cand_ref.shape[1]
    head = dense_ref.shape[0] - 2 * SLOTS - (total if last else main)
    turn = turn_ref[0]
    sources = arrivals()[:peers]
    start = jnp.int32(0)
    done = jnp.int32(0)
    starts, heres = [], []
    for a in range(peers):
        if a == earlier:
            done = jnp.minimum(start, turn_ref[1])
        here = jnp.clip(counts_ref[0, sources[a]] - turn * CAP, 0, CAP)
        starts.append(start)
        heres.append(here)
        start = start + here
    stop = start if last else jnp.minimum(start, main)

    dense_ref[...] = jnp.zeros_like(dense_ref)
    acc_ref[...] = jnp.zeros_like(acc_ref)
    q = iota((1, 2 * SLOTS), 1)
    for a in range(0, peers, 2):

        @pl.when((starts[a] < stop) & (starts[a + 1] + heres[a + 1] > done))
        def _():
            row = jnp.where(q < SLOTS, q + starts[a], q - SLOTS + starts[a + 1])
            ends = jnp.where(q < SLOTS, starts[a] + heres[a], starts[a + 1] + heres[a + 1])
            good = (row < ends) & (row >= done) & (row < stop)
            target = jnp.where(good, row - done, -1)
            base = pl.multiple_of(jnp.maximum(starts[a] - done, 0) // 16 * 16, 16)
            one = jnp.where(iota((2 * SLOTS, 1), 0) + base == target, 1.0, 0.0).astype(BF16)
            rows = jnp.dot(one, pairs[a // 2][...], preferred_element_type=F32)
            window = pl.ds(pl.multiple_of(base + head, 16), 2 * SLOTS)
            dense_ref[window, :] = (dense_ref[window, :].astype(F32) + rows).astype(BF16)

    there = jnp.int32(0)
    if last:
        q = iota((1, peers * CAP_CHOSEN), 1)
        target = jnp.full((1, peers * CAP_CHOSEN), -1, I32)
        for a in range(peers):
            here = jnp.clip(counts_ref[1, sources[a]] - turn * CAP_CHOSEN, 0, CAP_CHOSEN)
            slot = q - a * CAP_CHOSEN
            target = jnp.where((slot >= 0) & (slot < here), slot + there, target)
            there = there + here
        one = jnp.where(iota((head, 1), 0) == target, 1.0, 0.0).astype(BF16)
        rows = jnp.concatenate([pairs[a // 2][a % 2 * SLOTS + CAP : a % 2 * SLOTS + SLOTS, :] for a in range(peers)], axis=0)
        dense_ref[0:head, :] = jnp.dot(one, rows, preferred_element_type=F32).astype(BF16)

    sub = 256
    per = chunk // LANES
    low = jnp.where(iota((max(head, 8), 1), 0) < there, 0.0, -jnp.inf)

    def add_up(i, first, size, with_head, tiles):
        lines = pl.ds(pl.multiple_of(i * per, per), per)
        level = best_ref[lines, :]
        scaled = level * (1.0 / scale)
        for u in tiles:
            sims = lax.dot_general(dense_ref[pl.ds(first, size), :], slab_ref[pl.ds(pl.multiple_of(i * chunk + u * sub, sub), sub), :],
                                   (((1,), (1,)), ((), ())), preferred_element_type=F32)
            skip = head if with_head else 0
            part = acc_ref[pl.ds(first + skip, size - skip), :]
            for j in range(sub // LANES):
                k = u * (sub // LANES) + j
                cols = sims[:, j * LANES : (j + 1) * LANES]
                part += jnp.maximum(cols[skip:] - scaled[k : k + 1, :], 0.0)
                if with_head:
                    top = jnp.max(cols[:skip] + low, axis=0, keepdims=True) * scale
                    level_ref[pl.ds(i * per + k, 1), :] = jnp.maximum(level[k : k + 1, :], top)
            acc_ref[pl.ds(first + skip, size - skip), :] = part

    def main_step(i, carry):
        add_up(i, 0, head + main, last, range(chunk // sub))
        return carry

    lax.fori_loop(0, chunks, main_step, 0)

    slab = lax.shift_right_arithmetic(cand_ref[...], shift)
    slot = rank_ref[...] - turn * CAP
    place = jnp.full(slot.shape, -1, I32)
    for a in range(peers):
        place = jnp.where(slab == sources[a], slot + starts[a] - done, place)
    good = (slot >= 0) & (slot < CAP) & (place >= 0) & (place < stop - done)
    place = jnp.where(good, place, -1)

    def hand_out(ref, first, size):
        sums = jnp.sum(acc_ref[pl.ds(head + first, size), :], axis=1, keepdims=True) * scale
        at = iota((size, LANES), 0) + first
        for j in range(slot.shape[0]):
            mine = jnp.where(at == place[j : j + 1, :], sums, 0.0)
            out_ref[j : j + 1, :] = ref[j : j + 1, :] + jnp.sum(mine, axis=0, keepdims=True)

    hand_out(before_ref, 0, main)
    if last and total > main:

        @pl.when(stop - done > main)
        def _():
            def rest_step(k, carry):
                lines = sub // LANES
                edges = best_ref[pl.ds(k * lines, lines), :] * (1.0 / scale)
                tall = slab_ref[pl.ds(pl.multiple_of(k * sub, sub), sub), :]
                sims = lax.dot_general(dense_ref[pl.ds(head + main, total - main), :], tall,
                                       (((1,), (1,)), ((), ())), preferred_element_type=F32)
                for j in range(lines):
                    cols = sims[:, j * LANES : (j + 1) * LANES]
                    acc_ref[pl.ds(head + main, total - main), :] += jnp.maximum(cols - edges[j : j + 1, :], 0.0)
                return carry

            lax.fori_loop(0, chunks * (chunk // sub), rest_step, 0)
            hand_out(out_ref, main, total - main)


def gain(turn, counts, cand, rank, before, best, slab, pairs, earlier, main, chosen, scale):
    count, width = slab.shape
    total = cand.shape[0] * cand.shape[1]
    peers = 2 * len(pairs)
    last = chosen > 0
    body = lambda *refs: gain_kernel(*refs, peers=peers, earlier=earlier, main=main, last=last, scale=scale)
    vmem = pl.BlockSpec(memory_space=pltpu.VMEM)
    outs = [jax.ShapeDtypeStruct(cand.shape, F32)] + [jax.ShapeDtypeStruct(best.shape, F32)] * last
    rows = chosen + (total if last else main)
    made = pl.pallas_call(
        body,
        in_specs=[pl.BlockSpec(memory_space=pltpu.SMEM)] * 2 + [vmem] * 4
        + [vmem] + [vmem] * len(pairs),
        out_specs=[vmem] * len(outs),
        out_shape=outs,
        scratch_shapes=[pltpu.VMEM((rows + 2 * SLOTS, width), BF16),
                        pltpu.VMEM((rows, LANES), F32)],
        compiler_params=pltpu.CompilerParams(vmem_limit_bytes=24 * 2**20),
        cost_estimate=pl.CostEstimate(flops=2 * count * width * (main + chosen), transcendentals=0,
                                      bytes_accessed=2 * count * width),
        name="gain_last" if last else "gain",
    )(turn, counts, cand, rank, before, best, slab, *pairs)
    return made if last else made[0]


def device(x, y, c):
    return (x % 4) * 4 + y * 2 + c


def moved(array, dx, dy, dc):
    pairs = [(device(x, y, c), device(x + (dx if c == 0 else -dx), y ^ dy, c ^ dc))
             for x in range(4) for y in range(2) for c in range(2)]
    return lax.ppermute(array, "ground", pairs)


def arrivals():
    me = lax.axis_index("ground")
    x, y, c = me // 4, me // 2 % 2, me % 2
    sign = 1 - 2 * c
    near = [(0, y), (-sign, y), (sign, y), (0, 1 - y)]
    far = [(2, y), (sign, 1 - y), (-sign, 1 - y), (2, 1 - y)]
    here = lambda places: [(x + dx + 4) % 4 * 4 + yy * 2 + c for dx, yy in places]
    there = lambda places: [(x - dx + 4) % 4 * 4 + yy * 2 + 1 - c for dx, yy in places]
    return here(near) + there(near) + here(far) + there(far)


def join_kernel(own_ref, ahead_ref, behind_ref, flip_ref, first_ref, second_ref):
    first_ref[0:SLOTS, :] = own_ref[...]
    first_ref[SLOTS : 2 * SLOTS, :] = ahead_ref[...]
    second_ref[0:SLOTS, :] = behind_ref[...]
    second_ref[SLOTS : 2 * SLOTS, :] = flip_ref[...]


def join(*blocks):
    vmem = pl.BlockSpec(memory_space=pltpu.VMEM)
    pair = pltpu.VMEM((2 * SLOTS, blocks[0].shape[1]), BF16)
    return pl.pallas_call(join_kernel, in_specs=[vmem] * 4, out_specs=[vmem] * 2, out_shape=[pair] * 2, name="join",
                          compiler_params=pltpu.CompilerParams(vmem_limit_bytes=8 * 2**20))(*blocks)


def near_pairs(own):
    ahead = moved(own, 1, 0, 0)
    behind = moved(own, -1, 0, 0)
    flip = moved(own, 0, 1, 0)
    return join(own, ahead, behind, flip)


def far_pairs(near):
    first, second = near
    return [moved(second, -1, 0, 0), moved(first, 1, 1, 0)]


def both_cores(pairs):
    return list(pairs) + [moved(pair, 0, 0, 1) for pair in pairs]


def body(ground_rows, best, cand_index, chosen_index):
    count, width = ground_rows.shape
    scale = width ** (-0.5)
    peers = lax.axis_size("ground")
    whole = count * peers
    cand = cand_index.reshape(-1, LANES)
    chosen = chosen_index.reshape(1, -1)
    level = best.reshape(-1, LANES)
    total = cand_index.shape[0]
    first_rows = total * 13 // 32

    def finish(turn, limit, counts, rank, gains, level, pairs):
        state = jnp.stack([turn, limit]).astype(I32)
        return gain(state, counts, cand, rank, gains, level, ground_rows, pairs, peers // 2,
                    total - first_rows, chosen.shape[1], scale)

    block, rank, counts = pick(jnp.zeros((1,), I32), cand, chosen, ground_rows)
    turns = counts[2, 0]
    near = near_pairs(block)
    far = far_pairs(near)
    near = both_cores(near)
    gains = gain(jnp.zeros((2,), I32), counts, cand, rank, jnp.zeros(cand.shape, F32), level, ground_rows, near,
                 0, first_rows, 0, scale)
    gains, far = lax.optimization_barrier((gains, far))
    gains, new = finish(jnp.int32(0), jnp.int32(first_rows), counts, rank, gains, level, near + both_cores(far))

    def more(state):
        return state[0] < turns

    def again(state):
        turn, gains, new = state
        block, rank, counts = pick(turn.reshape(1), cand, chosen, ground_rows)
        near = near_pairs(block)
        pairs = both_cores(near) + both_cores(far_pairs(near))
        added, raised = finish(turn, jnp.int32(0), counts, rank, gains, level, pairs)
        return turn + 1, added, jnp.maximum(new, raised)

    _, gains, new = lax.while_loop(more, again, (jnp.int32(1), gains, new))
    blocks = gains.reshape(peers, -1) / whole
    arrived = lax.all_to_all(blocks, "ground", 0, 0, tiled=True)
    return arrived.sum(axis=0), new.reshape(-1)


def solution(mesh):
    in_specs = (P("ground", None), P("ground"), P("cand"), P())
    out_specs = (P(("cand", "ground")), P("ground"))
    return jax.shard_map(body, mesh=mesh, in_specs=in_specs, out_specs=out_specs, check_vma=False)
```

```python
import jax
import jax.numpy as jnp
from jax import lax
from jax.experimental import pallas as pl
from jax.experimental.pallas import tpu as pltpu
from jax.sharding import PartitionSpec as P


CAP = 96
CAP_CHOSEN = 16
SLOTS = CAP + CAP_CHOSEN
LANES = 128
TILE = 8

F32 = jnp.float32
BF16 = jnp.bfloat16
I32 = jnp.int32


def iota(shape, dim):
    return lax.broadcasted_iota(I32, shape, dim)


def pick_kernel(turn_ref, cand_ref, chosen_ref, slab_ref, block_ref, rank_ref, counts_ref,
                pad_ref, list_ref, slots_ref, stage_ref, sem, list_sem):
    count = slab_ref.shape[0]
    shift = count.bit_length() - 1
    me = lax.axis_index("ground")
    turn = turn_ref[0]
    rows = cand_ref.shape[0]
    lane = iota((LANES, LANES), 1)
    line = iota((LANES, LANES), 0)
    upper = jnp.where(line <= lane, 1.0, 0.0).astype(BF16)

    pad_ref[...] = jnp.full(pad_ref.shape, -1, I32)
    pad_ref[0:1, 0 : chosen_ref.shape[1]] = chosen_ref[...]
    index = jnp.concatenate([cand_ref[...], pad_ref[...]], axis=0)
    mine = lax.shift_right_arithmetic(index, shift) == me
    upto = jnp.dot(jnp.where(mine, 1.0, 0.0).astype(BF16), upper, preferred_element_type=F32)
    ends = jnp.broadcast_to(upto[:, LANES - 1 : LANES], upto.shape)
    before = jnp.zeros((1, LANES), F32)
    lines = []
    for j in range(rows):
        lines.append(before)
        before = before + ends[j : j + 1, :]
    ahead = jnp.concatenate(lines + [jnp.zeros((8, LANES), F32)], axis=0)
    slot = (upto - 1.0 + ahead).astype(I32)
    top = iota(index.shape, 0) < rows
    slot = slot - turn * jnp.where(top, CAP, CAP_CHOSEN)
    inside = mine & (slot >= 0) & (slot < jnp.where(top, CAP, CAP_CHOSEN))
    slot = jnp.where(inside, jnp.where(top, slot, slot + CAP), -1)
    packed = jnp.where(inside, index - me * count, 0)
    slot_t = slot.T
    packed_t = packed.T
    found = jnp.zeros((LANES, LANES), I32)
    for j in range(rows + 1):
        found += jnp.where(slot_t[:, j : j + 1] == lane, packed_t[:, j : j + 1], 0)
    row = jnp.sum(found.astype(F32), axis=0, keepdims=True)
    row = jnp.broadcast_to(row, (8, LANES))
    list_ref[...] = row.astype(I32)
    copy = pltpu.make_async_copy(list_ref, slots_ref, list_sem)
    copy.start()
    copy.wait()
    for p in range(SLOTS):
        tile = lax.shift_right_logical(slots_ref[0, p], 3)
        pltpu.make_async_copy(slab_ref.at[pl.ds(pl.multiple_of(tile * TILE, TILE), TILE), :],
                              stage_ref.at[pl.ds(p * TILE, TILE), :], sem).start()

    lower = jnp.where(line >= lane, 1.0, 0.0).astype(BF16)
    index_t = index.T

    def ranked(col, carry):
        hot = lax.shift_right_arithmetic(col, shift) == lane
        upto = jnp.dot(lower, jnp.where(hot, 1.0, 0.0).astype(BF16), preferred_element_type=F32)
        rank = jnp.sum(jnp.where(hot, upto - 1.0 + carry, 0.0), axis=1, keepdims=True)
        return rank, carry + upto[LANES - 1 : LANES, :]

    counts = jnp.zeros((1, LANES), F32)
    ranks = []
    for j in range(rows):
        rank, counts = ranked(index_t[:, j : j + 1], counts)
        ranks.append(rank)
    rank_ref[...] = jnp.concatenate(ranks, axis=1).T.astype(I32)
    _, ccounts = ranked(index_t[:, rows : rows + 1], jnp.zeros((1, LANES), F32))
    turns = jnp.maximum(
        (jnp.max(counts, axis=1, keepdims=True).astype(I32) + CAP - 1) // CAP,
        (jnp.max(ccounts, axis=1, keepdims=True).astype(I32) + CAP_CHOSEN - 1) // CAP_CHOSEN,
    )
    counts_ref[0:1, :] = counts.astype(I32)
    counts_ref[1:2, :] = ccounts.astype(I32)
    counts_ref[2:3, :] = jnp.broadcast_to(turns, (1, LANES))

    inner = row.T[:, 0:1].astype(I32) & (TILE - 1)
    want = inner[:SLOTS] + TILE * iota((SLOTS, 1), 0)
    one = jnp.where(iota((SLOTS, SLOTS * TILE), 1) == want, 1.0, 0.0).astype(BF16)
    pltpu.make_async_copy(slab_ref.at[pl.ds(0, SLOTS * TILE), :], stage_ref, sem).wait()
    block_ref[...] = jnp.dot(one, stage_ref[...], preferred_element_type=F32).astype(BF16)


def pick(turn, cand, chosen, slab):
    width = slab.shape[1]
    return pl.pallas_call(
        pick_kernel,
        in_specs=[pl.BlockSpec(memory_space=pltpu.SMEM), pl.BlockSpec(memory_space=pltpu.VMEM),
                  pl.BlockSpec(memory_space=pltpu.VMEM), pl.BlockSpec(memory_space=pl.ANY)],
        out_specs=[pl.BlockSpec(memory_space=pltpu.VMEM)] * 3,
        out_shape=[pltpu.VMEM((SLOTS, width), BF16), pltpu.VMEM(cand.shape, I32), pltpu.VMEM((8, LANES), I32)],
        scratch_shapes=[pltpu.VMEM((8, LANES), I32), pltpu.VMEM((8, LANES), I32),
                        pltpu.SMEM((8, LANES), I32), pltpu.VMEM((SLOTS * TILE, width), BF16),
                        pltpu.SemaphoreType.DMA, pltpu.SemaphoreType.DMA],
        compiler_params=pltpu.CompilerParams(vmem_limit_bytes=16 * 2**20),
        name="pick",
    )(turn, cand, chosen, slab)


def gain_kernel(turn_ref, counts_ref, cand_ref, rank_ref, before_ref, best_ref, floor_ref, slab_ref, *rest,
                peers, earlier, main, last, scale):
    pairs = rest[: peers // 2]
    rest = rest[peers // 2 :]
    if last:
        out_ref, level_ref, dense_ref, acc_ref, tall_ref, sems = rest
    else:
        out_ref, level_ref, dense_ref, acc_ref = rest
        level_ref[...] = floor_ref[...]
    count, _ = slab_ref.shape
    chunk = min(2048, count)
    chunks = count // chunk
    shift = count.bit_length() - 1
    total = cand_ref.shape[0] * cand_ref.shape[1]
    head = dense_ref.shape[0] - 2 * SLOTS - (total if last else main)
    turn = turn_ref[0]
    tall = slab_ref
    if last:
        tall = tall_ref
        for i in range(chunks):
            part = pl.ds(i * chunk, chunk)
            pltpu.make_async_copy(slab_ref.at[part, :], tall_ref.at[part, :], sems.at[i]).start()

    sources = arrivals()[:peers]
    start = jnp.int32(0)
    done = jnp.int32(0)
    starts, heres = [], []
    for a in range(peers):
        if a == earlier:
            done = jnp.minimum(start, turn_ref[1])
        here = jnp.clip(counts_ref[0, sources[a]] - turn * CAP, 0, CAP)
        starts.append(start)
        heres.append(here)
        start = start + here
    stop = start if last else jnp.minimum(start, main)

    dense_ref[...] = jnp.zeros_like(dense_ref)
    acc_ref[...] = jnp.zeros_like(acc_ref)
    q = iota((1, 2 * SLOTS), 1)
    for a in range(0, peers, 2):

        @pl.when((starts[a] < stop) & (starts[a + 1] + heres[a + 1] > done))
        def _():
            row = jnp.where(q < SLOTS, q + starts[a], q - SLOTS + starts[a + 1])
            ends = jnp.where(q < SLOTS, starts[a] + heres[a], starts[a + 1] + heres[a + 1])
            good = (row < ends) & (row >= done) & (row < stop)
            target = jnp.where(good, row - done, -1)
            base = pl.multiple_of(jnp.maximum(starts[a] - done, 0) // 16 * 16, 16)
            one = jnp.where(iota((2 * SLOTS, 1), 0) + base == target, 1.0, 0.0).astype(BF16)
            rows = jnp.dot(one, pairs[a // 2][...], preferred_element_type=F32)
            window = pl.ds(pl.multiple_of(base + head, 16), 2 * SLOTS)
            dense_ref[window, :] = (dense_ref[window, :].astype(F32) + rows).astype(BF16)

    there = jnp.int32(0)
    if last:
        q = iota((1, peers * CAP_CHOSEN), 1)
        target = jnp.full((1, peers * CAP_CHOSEN), -1, I32)
        for a in range(peers):
            here = jnp.clip(counts_ref[1, sources[a]] - turn * CAP_CHOSEN, 0, CAP_CHOSEN)
            slot = q - a * CAP_CHOSEN
            target = jnp.where((slot >= 0) & (slot < here), slot + there, target)
            there = there + here
        one = jnp.where(iota((head, 1), 0) == target, 1.0, 0.0).astype(BF16)
        rows = jnp.concatenate([pairs[a // 2][a % 2 * SLOTS + CAP : a % 2 * SLOTS + SLOTS, :] for a in range(peers)], axis=0)
        dense_ref[0:head, :] = jnp.dot(one, rows, preferred_element_type=F32).astype(BF16)

    sub = 256
    per = chunk // LANES
    low = jnp.where(iota((max(head, 8), 1), 0) < there, 0.0, -jnp.inf)

    def add_up(i, first, size, with_head, tiles):
        lines = pl.ds(pl.multiple_of(i * per, per), per)
        level = best_ref[lines, :]
        scaled = level * (1.0 / scale)
        for u in tiles:
            sims = lax.dot_general(dense_ref[pl.ds(first, size), :], tall[pl.ds(pl.multiple_of(i * chunk + u * sub, sub), sub), :],
                                   (((1,), (1,)), ((), ())), preferred_element_type=F32)
            skip = head if with_head else 0
            part = acc_ref[pl.ds(first + skip, size - skip), :]
            for j in range(sub // LANES):
                k = u * (sub // LANES) + j
                cols = sims[:, j * LANES : (j + 1) * LANES]
                part += jnp.maximum(cols[skip:] - scaled[k : k + 1, :], 0.0)
                if with_head:
                    top = jnp.max(cols[:skip] + low, axis=0, keepdims=True) * scale
                    line = pl.ds(i * per + k, 1)
                    level_ref[line, :] = jnp.maximum(floor_ref[line, :], top)
            acc_ref[pl.ds(first + skip, size - skip), :] = part

    def main_step(i, carry):
        if last:
            part = pl.ds(pl.multiple_of(i * chunk, chunk), chunk)
            pltpu.make_async_copy(slab_ref.at[part, :], tall_ref.at[part, :], sems.at[i]).wait()
        add_up(i, 0, head + main, last, range(chunk // sub))
        return carry

    lax.fori_loop(0, chunks, main_step, 0)

    slab = lax.shift_right_arithmetic(cand_ref[...], shift)
    slot = rank_ref[...] - turn * CAP
    place = jnp.full(slot.shape, -1, I32)
    for a in range(peers):
        place = jnp.where(slab == sources[a], slot + starts[a] - done, place)
    good = (slot >= 0) & (slot < CAP) & (place >= 0) & (place < stop - done)
    place = jnp.where(good, place, -1)

    def hand_out(ref, first, size):
        sums = jnp.sum(acc_ref[pl.ds(head + first, size), :], axis=1, keepdims=True) * scale
        at = iota((size, LANES), 0) + first
        for j in range(slot.shape[0]):
            mine = jnp.where(at == place[j : j + 1, :], sums, 0.0)
            out_ref[j : j + 1, :] = ref[j : j + 1, :] + jnp.sum(mine, axis=0, keepdims=True)

    hand_out(before_ref, 0, main)
    if last and total > main:

        @pl.when(stop - done > main)
        def _():
            def rest_step(k, carry):
                lines = sub // LANES
                edges = best_ref[pl.ds(k * lines, lines), :] * (1.0 / scale)
                rows = tall[pl.ds(pl.multiple_of(k * sub, sub), sub), :]
                sims = lax.dot_general(dense_ref[pl.ds(head + main, total - main), :], rows,
                                       (((1,), (1,)), ((), ())), preferred_element_type=F32)
                for j in range(lines):
                    cols = sims[:, j * LANES : (j + 1) * LANES]
                    acc_ref[pl.ds(head + main, total - main), :] += jnp.maximum(cols - edges[j : j + 1, :], 0.0)
                return carry

            lax.fori_loop(0, chunks * (chunk // sub), rest_step, 0)
            hand_out(out_ref, main, total - main)


def gain(turn, counts, cand, rank, before, best, floor, slab, pairs, earlier, main, chosen, scale):
    count, width = slab.shape
    total = cand.shape[0] * cand.shape[1]
    peers = 2 * len(pairs)
    last = chosen > 0
    chunk = min(2048, count)
    copies = [pltpu.VMEM(slab.shape, BF16), pltpu.SemaphoreType.DMA((count // chunk,))] * last
    body = lambda *refs: gain_kernel(*refs, peers=peers, earlier=earlier, main=main, last=last, scale=scale)
    vmem = pl.BlockSpec(memory_space=pltpu.VMEM)
    outs = [jax.ShapeDtypeStruct(cand.shape, F32), jax.ShapeDtypeStruct(best.shape, F32)]
    rows = chosen + (total if last else main)
    return pl.pallas_call(
        body,
        in_specs=[pl.BlockSpec(memory_space=pltpu.SMEM)] * 2 + [vmem] * 5
        + [pl.BlockSpec(memory_space=pl.ANY) if last else vmem] + [vmem] * len(pairs),
        out_specs=[vmem] * len(outs),
        out_shape=outs,
        scratch_shapes=[pltpu.VMEM((rows + 2 * SLOTS, width), BF16),
                        pltpu.VMEM((rows, LANES), F32),
                        *copies],
        compiler_params=pltpu.CompilerParams(vmem_limit_bytes=(40 if last else 24) * 2**20),
        cost_estimate=pl.CostEstimate(flops=2 * count * width * (main + chosen), transcendentals=0,
                                      bytes_accessed=2 * count * width),
        name="gain_last" if last else "gain",
    )(turn, counts, cand, rank, before, best, floor, slab, *pairs)


def device(x, y, c):
    return (x % 4) * 4 + y * 2 + c


def moved(array, dx, dy, dc):
    pairs = [(device(x, y, c), device(x + (dx if c == 0 else -dx), y ^ dy, c ^ dc))
             for x in range(4) for y in range(2) for c in range(2)]
    return lax.ppermute(array, "ground", pairs)


def arrivals():
    me = lax.axis_index("ground")
    x, y, c = me // 4, me // 2 % 2, me % 2
    sign = 1 - 2 * c
    near = [(0, y), (-sign, y), (sign, y), (0, 1 - y)]
    far = [(2, y), (sign, 1 - y), (-sign, 1 - y), (2, 1 - y)]
    here = lambda places: [(x + dx + 4) % 4 * 4 + yy * 2 + c for dx, yy in places]
    there = lambda places: [(x - dx + 4) % 4 * 4 + yy * 2 + 1 - c for dx, yy in places]
    return here(near) + there(near) + here(far) + there(far)


def join_kernel(own_ref, ahead_ref, behind_ref, flip_ref, first_ref, second_ref):
    first_ref[0:SLOTS, :] = own_ref[...]
    first_ref[SLOTS : 2 * SLOTS, :] = ahead_ref[...]
    second_ref[0:SLOTS, :] = behind_ref[...]
    second_ref[SLOTS : 2 * SLOTS, :] = flip_ref[...]


def join(*blocks):
    vmem = pl.BlockSpec(memory_space=pltpu.VMEM)
    pair = pltpu.VMEM((2 * SLOTS, blocks[0].shape[1]), BF16)
    return pl.pallas_call(join_kernel, in_specs=[vmem] * 4, out_specs=[vmem] * 2, out_shape=[pair] * 2, name="join",
                          compiler_params=pltpu.CompilerParams(vmem_limit_bytes=8 * 2**20))(*blocks)


def near_pairs(own):
    ahead = moved(own, 1, 0, 0)
    behind = moved(own, -1, 0, 0)
    flip = moved(own, 0, 1, 0)
    return join(own, ahead, behind, flip)


def far_pairs(near):
    first, second = near
    return [moved(second, -1, 0, 0), moved(first, 1, 1, 0)]


def both_cores(pairs):
    return list(pairs) + [moved(pair, 0, 0, 1) for pair in pairs]


def body(ground_rows, best, cand_index, chosen_index):
    count, width = ground_rows.shape
    scale = width ** (-0.5)
    peers = lax.axis_size("ground")
    whole = count * peers
    cand = cand_index.reshape(-1, LANES)
    chosen = chosen_index.reshape(1, -1)
    level = best.reshape(-1, LANES)
    total = cand_index.shape[0]
    first_rows = total * 7 // 16

    def finish(turn, limit, counts, rank, gains, floor, pairs):
        state = jnp.stack([turn, limit]).astype(I32)
        return gain(state, counts, cand, rank, gains, level, floor, ground_rows, pairs, peers // 2,
                    total - first_rows, chosen.shape[1], scale)

    block, rank, counts = pick(jnp.zeros((1,), I32), cand, chosen, ground_rows)
    turns = counts[2, 0]
    near = near_pairs(block)
    far = far_pairs(near)
    near = both_cores(near)
    gains, unused = gain(jnp.zeros((2,), I32), counts, cand, rank, jnp.zeros(cand.shape, F32), level, level,
                      ground_rows, near, 0, first_rows, 0, scale)
    gains, far = lax.optimization_barrier((gains, far))
    gains, new = finish(jnp.int32(0), jnp.int32(first_rows), counts, rank, gains, level, near + both_cores(far))

    def more(state):
        return state[0] < turns

    def again(state):
        turn, gains, new = state
        block, rank, counts = pick(turn.reshape(1), cand, chosen, ground_rows)
        near = near_pairs(block)
        pairs = both_cores(near) + both_cores(far_pairs(near))
        gains, new = finish(turn, jnp.int32(0), counts, rank, gains, new, pairs)
        return turn + 1, gains, new

    unused, gains, new = lax.while_loop(more, again, (jnp.int32(1), gains, new))
    blocks = gains.reshape(peers, -1) / whole
    arrived = lax.all_to_all(blocks, "ground", 0, 0, tiled=True)
    return arrived.sum(axis=0), new.reshape(-1)


def solution(mesh):
    in_specs = (P("ground", None), P("ground"), P("cand"), P())
    out_specs = (P(("cand", "ground")), P("ground"))
    return jax.shard_map(body, mesh=mesh, in_specs=in_specs, out_specs=out_specs, check_vma=False)
```

```python
import jax
import jax.numpy as jnp
from jax import lax
from jax.experimental import pallas as pl
from jax.experimental.pallas import tpu as pltpu
from jax.sharding import PartitionSpec as P


SLOTS = 104
CAP_CHOSEN = 16
WINDOW = 2 * SLOTS + 16
LANES = 128
TILE = 8

F32 = jnp.float32
BF16 = jnp.bfloat16
I32 = jnp.int32


def iota(shape, dim):
    return lax.broadcasted_iota(I32, shape, dim)


def sent_and_room(turn, chosen):
    before = turn * CAP_CHOSEN
    return SLOTS * turn - jnp.minimum(chosen, before), SLOTS - jnp.clip(chosen - before, 0, CAP_CHOSEN)


def pick_kernel(turn_ref, cand_ref, chosen_ref, slab_ref, block_ref, rank_ref, counts_ref,
                pad_ref, list_ref, slots_ref, stage_ref, sem, list_sem):
    count = slab_ref.shape[0]
    shift = count.bit_length() - 1
    me = lax.axis_index("ground")
    turn = turn_ref[0]
    rows = cand_ref.shape[0]
    lane = iota((LANES, LANES), 1)
    line = iota((LANES, LANES), 0)
    upper = jnp.where(line <= lane, 1.0, 0.0).astype(BF16)

    pad_ref[...] = jnp.full(pad_ref.shape, -1, I32)
    pad_ref[0:1, 0 : chosen_ref.shape[1]] = chosen_ref[...]
    index = jnp.concatenate([cand_ref[...], pad_ref[...]], axis=0)
    mine = lax.shift_right_arithmetic(index, shift) == me
    upto = jnp.dot(jnp.where(mine, 1.0, 0.0).astype(BF16), upper, preferred_element_type=F32)
    ends = jnp.broadcast_to(upto[:, LANES - 1 : LANES], upto.shape)
    before = jnp.zeros((1, LANES), F32)
    lines = []
    for j in range(rows):
        lines.append(before)
        before = before + ends[j : j + 1, :]
    ahead = jnp.concatenate(lines + [jnp.zeros((8, LANES), F32)], axis=0)
    slot = (upto - 1.0 + ahead).astype(I32)
    top = iota(index.shape, 0) < rows
    chosen_here = upto[rows : rows + 1, LANES - 1 : LANES].astype(I32)
    sent, room = sent_and_room(turn, chosen_here)
    slot = slot - jnp.where(top, sent, turn * CAP_CHOSEN)
    inside = mine & (slot >= 0) & (slot < jnp.where(top, room, CAP_CHOSEN))
    slot = jnp.where(inside, jnp.where(top, slot, SLOTS - 1 - slot), -1)
    packed = jnp.where(inside, index - me * count, 0)
    slot_t = slot.T
    packed_t = packed.T
    found = jnp.zeros((LANES, LANES), I32)
    for j in range(rows + 1):
        found += jnp.where(slot_t[:, j : j + 1] == lane, packed_t[:, j : j + 1], 0)
    row = jnp.sum(found.astype(F32), axis=0, keepdims=True)
    row = jnp.broadcast_to(row, (8, LANES))
    list_ref[...] = row.astype(I32)
    copy = pltpu.make_async_copy(list_ref, slots_ref, list_sem)
    copy.start()
    copy.wait()
    for p in range(SLOTS):
        tile = lax.shift_right_logical(slots_ref[0, p], 3)
        pltpu.make_async_copy(slab_ref.at[pl.ds(pl.multiple_of(tile * TILE, TILE), TILE), :],
                              stage_ref.at[pl.ds(p * TILE, TILE), :], sem).start()

    lower = jnp.where(line >= lane, 1.0, 0.0).astype(BF16)
    index_t = index.T

    def ranked(col, carry):
        hot = lax.shift_right_arithmetic(col, shift) == lane
        upto = jnp.dot(lower, jnp.where(hot, 1.0, 0.0).astype(BF16), preferred_element_type=F32)
        rank = jnp.sum(jnp.where(hot, upto - 1.0 + carry, 0.0), axis=1, keepdims=True)
        return rank, carry + upto[LANES - 1 : LANES, :]

    counts = jnp.zeros((1, LANES), F32)
    ranks = []
    for j in range(rows):
        rank, counts = ranked(index_t[:, j : j + 1], counts)
        ranks.append(rank)
    rank_ref[...] = jnp.concatenate(ranks, axis=1).T.astype(I32)
    _, ccounts = ranked(index_t[:, rows : rows + 1], jnp.zeros((1, LANES), F32))
    turns = jnp.maximum(
        (jnp.max(counts + ccounts, axis=1, keepdims=True).astype(I32) + SLOTS - 1) // SLOTS,
        (jnp.max(ccounts, axis=1, keepdims=True).astype(I32) + CAP_CHOSEN - 1) // CAP_CHOSEN,
    )
    counts_ref[0:1, :] = counts.astype(I32)
    counts_ref[1:2, :] = ccounts.astype(I32)
    counts_ref[2:3, :] = jnp.broadcast_to(turns, (1, LANES))

    inner = row.T[:, 0:1].astype(I32) & (TILE - 1)
    want = inner[:SLOTS] + TILE * iota((SLOTS, 1), 0)
    one = jnp.where(iota((SLOTS, SLOTS * TILE), 1) == want, 1.0, 0.0).astype(BF16)
    pltpu.make_async_copy(slab_ref.at[pl.ds(0, SLOTS * TILE), :], stage_ref, sem).wait()
    block_ref[...] = jnp.dot(one, stage_ref[...], preferred_element_type=F32).astype(BF16)


def pick(turn, cand, chosen, slab):
    width = slab.shape[1]
    return pl.pallas_call(
        pick_kernel,
        in_specs=[pl.BlockSpec(memory_space=pltpu.SMEM), pl.BlockSpec(memory_space=pltpu.VMEM),
                  pl.BlockSpec(memory_space=pltpu.VMEM), pl.BlockSpec(memory_space=pl.ANY)],
        out_specs=[pl.BlockSpec(memory_space=pltpu.VMEM)] * 3,
        out_shape=[pltpu.VMEM((SLOTS, width), BF16), pltpu.VMEM(cand.shape, I32), pltpu.VMEM((8, LANES), I32)],
        scratch_shapes=[pltpu.VMEM((8, LANES), I32), pltpu.VMEM((8, LANES), I32),
                        pltpu.SMEM((8, LANES), I32), pltpu.VMEM((SLOTS * TILE, width), BF16),
                        pltpu.SemaphoreType.DMA, pltpu.SemaphoreType.DMA],
        compiler_params=pltpu.CompilerParams(vmem_limit_bytes=16 * 2**20),
        name="pick",
    )(turn, cand, chosen, slab)


def gain_kernel(turn_ref, counts_ref, cand_ref, rank_ref, before_ref, best_ref, floor_ref, slab_ref, *rest,
                peers, earlier, main, last, scale):
    pairs = rest[: peers // 2]
    rest = rest[peers // 2 :]
    if last:
        out_ref, level_ref, dense_ref, acc_ref, tall_ref, sems = rest
    else:
        out_ref, level_ref, dense_ref, acc_ref = rest
        level_ref[...] = floor_ref[...]
    count, _ = slab_ref.shape
    chunk = min(2048 if last else 4096, count)
    chunks = count // chunk
    shift = count.bit_length() - 1
    total = cand_ref.shape[0] * cand_ref.shape[1]
    head = dense_ref.shape[0] - WINDOW - (total if last else main)
    turn = turn_ref[0]
    tall = slab_ref
    if last:
        tall = tall_ref
        for i in range(chunks):
            part = pl.ds(i * chunk, chunk)
            pltpu.make_async_copy(slab_ref.at[part, :], tall_ref.at[part, :], sems.at[i]).start()

    sources = arrivals()[:peers]
    start = jnp.int32(0)
    done = jnp.int32(0)
    starts, heres, sents = [], [], []
    for a in range(peers):
        if a == earlier:
            done = jnp.minimum(start, turn_ref[1])
        sent, room = sent_and_room(turn, counts_ref[1, sources[a]])
        here = jnp.clip(counts_ref[0, sources[a]] - sent, 0, room)
        starts.append(start)
        sents.append(sent)
        heres.append(here)
        start = start + here
    stop = start if last else jnp.minimum(start, main)

    dense_ref[...] = jnp.zeros_like(dense_ref)
    acc_ref[...] = jnp.zeros_like(acc_ref)
    q = iota((1, 2 * SLOTS), 1)

    def place_pair(a):
        row = jnp.where(q < SLOTS, q + starts[a], q - SLOTS + starts[a + 1])
        ends = jnp.where(q < SLOTS, starts[a] + heres[a], starts[a + 1] + heres[a + 1])
        good = (row < ends) & (row >= done) & (row < stop)
        target = jnp.where(good, row - done, -1)
        bound = total if last else main
        base = pl.multiple_of(jnp.clip(starts[a] - done, 0, bound) // 16 * 16, 16)
        one = jnp.where(iota((WINDOW, 1), 0) + base == target, 1.0, 0.0).astype(BF16)
        rows = jnp.dot(one, pairs[a // 2][...], preferred_element_type=F32)
        window = pl.ds(pl.multiple_of(base + head, 16), WINDOW)
        dense_ref[window, :] = (dense_ref[window, :].astype(F32) + rows).astype(BF16)

    for a in range(0, peers, 2):
        if a < earlier:
            pl.when(starts[a + 1] + heres[a + 1] > done)(lambda a=a: place_pair(a))
        else:
            place_pair(a)

    there = jnp.int32(0)
    if last:
        q = iota((1, peers * CAP_CHOSEN), 1)
        target = jnp.full((1, peers * CAP_CHOSEN), -1, I32)
        for a in range(peers):
            here = jnp.clip(counts_ref[1, sources[a]] - turn * CAP_CHOSEN, 0, CAP_CHOSEN)
            slot = (a + 1) * CAP_CHOSEN - 1 - q
            good = (slot >= 0) & (slot < here) & (slot < CAP_CHOSEN)
            target = jnp.where(good, slot + there, target)
            there = there + here
        one = jnp.where(iota((head, 1), 0) == target, 1.0, 0.0).astype(BF16)
        rows = jnp.concatenate([pairs[a // 2][(a % 2 + 1) * SLOTS - CAP_CHOSEN : (a % 2 + 1) * SLOTS, :] for a in range(peers)], axis=0)
        dense_ref[0:head, :] = jnp.dot(one, rows, preferred_element_type=F32).astype(BF16)

    sub = 256
    per = chunk // LANES
    low = jnp.where(iota((max(head, 8), 1), 0) < there, 0.0, -jnp.inf)

    def add_up(i, first, size, with_head, tiles):
        lines = pl.ds(pl.multiple_of(i * per, per), per)
        level = best_ref[lines, :]
        scaled = level * (1.0 / scale)
        for u in tiles:
            sims = lax.dot_general(dense_ref[pl.ds(first, size), :], tall[pl.ds(pl.multiple_of(i * chunk + u * sub, sub), sub), :],
                                   (((1,), (1,)), ((), ())), preferred_element_type=F32)
            skip = head if with_head else 0
            part = acc_ref[pl.ds(first + skip, size - skip), :]
            for j in range(sub // LANES):
                k = u * (sub // LANES) + j
                cols = sims[:, j * LANES : (j + 1) * LANES]
                part += jnp.maximum(cols[skip:] - scaled[k : k + 1, :], 0.0)
                if with_head:
                    top = jnp.max(cols[:skip] + low, axis=0, keepdims=True) * scale
                    line = pl.ds(i * per + k, 1)
                    level_ref[line, :] = jnp.maximum(floor_ref[line, :], top)
            acc_ref[pl.ds(first + skip, size - skip), :] = part

    def main_step(i, carry):
        if last:
            part = pl.ds(pl.multiple_of(i * chunk, chunk), chunk)
            pltpu.make_async_copy(slab_ref.at[part, :], tall_ref.at[part, :], sems.at[i]).wait()
        add_up(i, 0, head + main, last, range(chunk // sub))
        return carry

    lax.fori_loop(0, chunks, main_step, 0)

    slab = lax.shift_right_arithmetic(cand_ref[...], shift)
    place = jnp.full(slab.shape, -1, I32)
    for a in range(peers):
        slot = rank_ref[...] - sents[a]
        good = (slab == sources[a]) & (slot >= 0) & (slot < heres[a])
        place = jnp.where(good, slot + starts[a] - done, place)
    place = jnp.where((place >= 0) & (place < stop - done), place, -1)

    def hand_out(ref, first, size):
        sums = jnp.sum(acc_ref[pl.ds(head + first, size), :], axis=1, keepdims=True) * scale
        at = iota((size, LANES), 0) + first
        for j in range(place.shape[0]):
            mine = jnp.where(at == place[j : j + 1, :], sums, 0.0)
            out_ref[j : j + 1, :] = ref[j : j + 1, :] + jnp.sum(mine, axis=0, keepdims=True)

    hand_out(before_ref, 0, main)
    if last and total > main:

        @pl.when(stop - done > main)
        def _():
            def rest_step(k, carry):
                lines = sub // LANES
                edges = best_ref[pl.ds(k * lines, lines), :] * (1.0 / scale)
                rows = tall[pl.ds(pl.multiple_of(k * sub, sub), sub), :]
                sims = lax.dot_general(dense_ref[pl.ds(head + main, total - main), :], rows,
                                       (((1,), (1,)), ((), ())), preferred_element_type=F32)
                for j in range(lines):
                    cols = sims[:, j * LANES : (j + 1) * LANES]
                    acc_ref[pl.ds(head + main, total - main), :] += jnp.maximum(cols - edges[j : j + 1, :], 0.0)
                return carry

            lax.fori_loop(0, chunks * (chunk // sub), rest_step, 0)
            hand_out(out_ref, main, total - main)


def gain(turn, counts, cand, rank, before, best, floor, slab, pairs, earlier, main, chosen, scale):
    count, width = slab.shape
    total = cand.shape[0] * cand.shape[1]
    peers = 2 * len(pairs)
    last = chosen > 0
    chunk = min(2048, count)
    copies = [pltpu.VMEM(slab.shape, BF16), pltpu.SemaphoreType.DMA((count // chunk,))] * last
    body = lambda *refs: gain_kernel(*refs, peers=peers, earlier=earlier, main=main, last=last, scale=scale)
    vmem = pl.BlockSpec(memory_space=pltpu.VMEM)
    outs = [jax.ShapeDtypeStruct(cand.shape, F32), jax.ShapeDtypeStruct(best.shape, F32)]
    rows = chosen + (total if last else main)
    return pl.pallas_call(
        body,
        in_specs=[pl.BlockSpec(memory_space=pltpu.SMEM)] * 2 + [vmem] * 5
        + [pl.BlockSpec(memory_space=pl.ANY) if last else vmem] + [vmem] * len(pairs),
        out_specs=[vmem] * len(outs),
        out_shape=outs,
        scratch_shapes=[pltpu.VMEM((rows + WINDOW, width), BF16),
                        pltpu.VMEM((rows, LANES), F32),
                        *copies],
        compiler_params=pltpu.CompilerParams(vmem_limit_bytes=(40 if last else 24) * 2**20),
        cost_estimate=pl.CostEstimate(flops=2 * count * width * (main + chosen), transcendentals=0,
                                      bytes_accessed=2 * count * width),
        name="gain_last" if last else "gain",
    )(turn, counts, cand, rank, before, best, floor, slab, *pairs)


def device(x, y, c):
    return (x % 4) * 4 + y * 2 + c


def moved(array, dx, dy, dc):
    pairs = [(device(x, y, c), device(x + (dx if c == 0 else -dx), y ^ dy, c ^ dc))
             for x in range(4) for y in range(2) for c in range(2)]
    return lax.ppermute(array, "ground", pairs)


def arrivals():
    me = lax.axis_index("ground")
    x, y, c = me // 4, me // 2 % 2, me % 2
    sign = 1 - 2 * c
    near = [(0, y), (-sign, y), (sign, y), (0, 1 - y)]
    far = [(2, y), (sign, 1 - y), (-sign, 1 - y), (2, 1 - y)]
    here = lambda places: [(x + dx + 4) % 4 * 4 + yy * 2 + c for dx, yy in places]
    there = lambda places: [(x - dx + 4) % 4 * 4 + yy * 2 + 1 - c for dx, yy in places]
    return here(near) + there(near) + here(far) + there(far)


def join_kernel(own_ref, ahead_ref, behind_ref, flip_ref, first_ref, second_ref):
    first_ref[0:SLOTS, :] = own_ref[...]
    first_ref[SLOTS : 2 * SLOTS, :] = ahead_ref[...]
    second_ref[0:SLOTS, :] = behind_ref[...]
    second_ref[SLOTS : 2 * SLOTS, :] = flip_ref[...]


def join(*blocks):
    vmem = pl.BlockSpec(memory_space=pltpu.VMEM)
    pair = pltpu.VMEM((2 * SLOTS, blocks[0].shape[1]), BF16)
    return pl.pallas_call(join_kernel, in_specs=[vmem] * 4, out_specs=[vmem] * 2, out_shape=[pair] * 2, name="join",
                          compiler_params=pltpu.CompilerParams(vmem_limit_bytes=8 * 2**20))(*blocks)


def near_pairs(own):
    ahead = moved(own, 1, 0, 0)
    behind = moved(own, -1, 0, 0)
    flip = moved(own, 0, 1, 0)
    return join(own, ahead, behind, flip)


def far_pairs(near):
    first, second = near
    return [moved(second, -1, 0, 0), moved(first, 1, 1, 0)]


def both_cores(pairs):
    return list(pairs) + [moved(pair, 0, 0, 1) for pair in pairs]


def body(ground_rows, best, cand_index, chosen_index):
    count, width = ground_rows.shape
    scale = width ** (-0.5)
    peers = lax.axis_size("ground")
    whole = count * peers
    cand = cand_index.reshape(-1, LANES)
    chosen = chosen_index.reshape(1, -1)
    level = best.reshape(-1, LANES)
    total = cand_index.shape[0]
    first_rows = total * 7 // 16

    def finish(turn, limit, counts, rank, gains, floor, pairs):
        state = jnp.stack([turn, limit]).astype(I32)
        return gain(state, counts, cand, rank, gains, level, floor, ground_rows, pairs, peers // 2,
                    total - first_rows, chosen.shape[1], scale)

    block, rank, counts = pick(jnp.zeros((1,), I32), cand, chosen, ground_rows)
    turns = counts[2, 0]
    near = near_pairs(block)
    far = far_pairs(near)
    near = both_cores(near)
    gains, unused = gain(jnp.zeros((2,), I32), counts, cand, rank, jnp.zeros(cand.shape, F32), level, level,
                      ground_rows, near, 0, first_rows, 0, scale)
    gains, far = lax.optimization_barrier((gains, far))
    gains, new = finish(jnp.int32(0), jnp.int32(first_rows), counts, rank, gains, level, near + both_cores(far))

    def more(state):
        return state[0] < turns

    def again(state):
        turn, gains, new = state
        block, rank, counts = pick(turn.reshape(1), cand, chosen, ground_rows)
        near = near_pairs(block)
        pairs = both_cores(near) + both_cores(far_pairs(near))
        gains, new = finish(turn, jnp.int32(0), counts, rank, gains, new, pairs)
        return turn + 1, gains, new

    unused, gains, new = lax.while_loop(more, again, (jnp.int32(1), gains, new))
    blocks = gains.reshape(peers, -1) / whole
    arrived = lax.all_to_all(blocks, "ground", 0, 0, tiled=True)
    return arrived.sum(axis=0), new.reshape(-1)


def solution(mesh):
    in_specs = (P("ground", None), P("ground"), P("cand"), P())
    out_specs = (P(("cand", "ground")), P("ground"))
    return jax.shard_map(body, mesh=mesh, in_specs=in_specs, out_specs=out_specs, check_vma=False)
```
